256 devices in a mesh: row: 8 (over x, y_lo), col: 32 (over y_hi, z, core).
Axes of the slice: x: 4, y: 4 (y_hi: 2, y_lo: 2; y = y_hi * 2 + y_lo), z: 8, core: 2. Of those that a mesh axis runs over, the one named last changes fastest.
Arguments:
- mlp_param: float32 [6144, 24576], P('row', 'col'), may hold values from -250 to 250
- mlp_grad: bfloat16 [6144, 24576], P('row', 'col'), may hold values from -250 to 250
- mlp_row_state: float32 [6144], P('row'), may hold values from 0.03 to 2.7
- mlp_col_state: float32 [24576], P('col'), may hold values from 0.02 to 0.3
- attn_param: float32 [6144, 6144], P('row', 'col'), may hold values from -250 to 250
- attn_grad: bfloat16 [6144, 6144], P('row', 'col'), may hold values from -250 to 250
- attn_row_state: float32 [6144], P('row'), may hold values from 0.03 to 2.7
- attn_col_state: float32 [6144], P('col'), may hold values from 0.02 to 0.3
Outputs:
- mlp_param_new: float32 [6144, 24576], P('row', 'col')
- attn_param_new: float32 [6144, 6144], P('row', 'col')
- mlp_row_new: float32 [6144], P('row')
- mlp_col_new: float32 [24576], P('col')
- attn_row_new: float32 [6144], P('row')
- attn_col_new: float32 [6144], P('col')
- attn_copy: bfloat16 [6144, 6144], P(None, 'col')
The draws below stay inside these ranges and needn't reach their ends.
All inputs are finite; a program needn't handle non-finite values.
Results may differ from the reference program's by a relative error of at most 0.0004.
Values may be sent and summed in bfloat16 or wider, within the bound.
No kernel may reach another device: no remote copies, remote signals or barrier semaphores. Data moves between devices by JAX's collectives and lax.ppermute only.
A program may use at most 64 MiB of HBM per device.

```python
import math
import jax
import jax.numpy as jnp
from jax import lax

D = 6144
FF = 24576
STEP = 4


def scaled_field(key, height, width, level):
    keys = jax.random.split(key, 3)
    base = jnp.clip(jax.random.normal(keys[0], (height, width), jnp.float32), -4.0, 4.0)
    overall = 1.0
    row_place = jnp.arange(height, dtype=jnp.float32) / height - 0.5
    col_place = jnp.arange(width, dtype=jnp.float32) / width - 0.5
    row_scale = jnp.exp(jax.random.uniform(keys[1], (height,), jnp.float32, -1.15, 1.15)) * jnp.power(3.0, row_place)
    col_scale = jnp.exp(jax.random.uniform(keys[2], (width,), jnp.float32, -1.15, 1.15)) * jnp.power(3.0, col_place)
    row_scale = row_scale / jnp.sqrt(jnp.mean(jnp.square(row_scale)))
    col_scale = col_scale / jnp.sqrt(jnp.mean(jnp.square(col_scale)))
    return level * overall * base * row_scale[:, None] * col_scale[None, :]


def falling_state(key, length):
    jitter = jax.random.uniform(key, (length,), jnp.float32, -0.69, 0.69)
    place = jnp.arange(length, dtype=jnp.float32) / length - 0.5
    return 0.3 * jnp.exp(jitter) * jnp.power(10.0, -place)


def draw_mlp_param(key, part):
    return scaled_field(jax.random.fold_in(key, 11), D, FF, 1.0)


def draw_mlp_grad(key, part):
    return scaled_field(jax.random.fold_in(key, 12), D, FF, 0.4).astype(jnp.bfloat16)


def draw_attn_param(key, part):
    return scaled_field(jax.random.fold_in(key, 13), D, D, 1.0)


def draw_attn_grad(key, part):
    return scaled_field(jax.random.fold_in(key, 14), D, D, 0.4).astype(jnp.bfloat16)


def draw_mlp_row_state(key, part):
    return falling_state(jax.random.fold_in(key, 21), D)


def draw_attn_row_state(key, part):
    return falling_state(jax.random.fold_in(key, 22), D)


def shard_levels(rng, extent, cuts, least, high):
    gain = 1.0
    for position, shards_of in cuts:
        steps = jax.random.uniform(jax.random.fold_in(jax.random.fold_in(rng, 6), position), (shards_of,), jnp.float32, least / len(cuts), high / len(cuts))
        gain = gain * jnp.repeat(jnp.exp(steps), extent[position] // shards_of).reshape((-1,) + (1,) * (len(extent) - 1 - position))
    return gain


def setup_inputs(seed: int = 0) -> dict:
    key_list = jax.random.split(jax.random.key(seed), 9)
    return {
        "mlp_param": draw_mlp_param(jax.random.fold_in(key_list[8], 71), 0),
        "mlp_grad": draw_mlp_grad(jax.random.fold_in(key_list[8], 71), 0),
        "mlp_row_state": draw_mlp_row_state(jax.random.fold_in(key_list[8], 71), 0),
        "mlp_col_state": jnp.clip(jnp.exp(math.log(0.3) - 2.7080503 * jax.random.uniform(key_list[3], (FF,), jnp.float32) ** shard_levels(key_list[3], (FF,), ((0, 32),), -0.2, 0.2)), 0.02, 0.3),
        "attn_param": draw_attn_param(jax.random.fold_in(key_list[8], 71), 0),
        "attn_grad": draw_attn_grad(jax.random.fold_in(key_list[8], 71), 0),
        "attn_row_state": draw_attn_row_state(jax.random.fold_in(key_list[8], 71), 0),
        "attn_col_state": jnp.clip(jnp.exp(math.log(0.3) - 2.7080503 * jax.random.uniform(key_list[7], (D,), jnp.float32) ** shard_levels(key_list[7], (D,), ((0, 32),), -0.2, 0.2)), 0.02, 0.3),
    }


TINY_SQUARE = 1e-30
LEARN_RATE = 0.05
DECAY_POWER = 0.8

def moments(grad, row_state, col_state):
    keep_rate = 1.0 - STEP ** (-DECAY_POWER)
    square = jnp.square(grad.astype(jnp.float32)) + TINY_SQUARE
    rows_new = keep_rate * row_state + (1.0 - keep_rate) * lax.optimization_barrier(jnp.mean(square, axis=1))
    cols_new = keep_rate * col_state + (1.0 - keep_rate) * lax.optimization_barrier(jnp.mean(square, axis=0))
    return (rows_new, cols_new)

def update_matrix(param, grad, rows_new, cols_new):
    raw = grad.astype(jnp.float32) / jnp.sqrt(rows_new[:, None] * cols_new[None, :])
    clip = jnp.maximum(1.0, jnp.sqrt(jnp.mean(jnp.square(raw))))
    step_size = LEARN_RATE * jnp.sqrt(jnp.mean(jnp.square(param)))
    return param - step_size * (raw / clip)

def reference(mlp_param, mlp_grad, mlp_row_state, mlp_col_state, attn_param, attn_grad, attn_row_state, attn_col_state):
    mlp_rows, mlp_cols = moments(mlp_grad, mlp_row_state, mlp_col_state)
    attn_rows, attn_cols = moments(attn_grad, attn_row_state, attn_col_state)
    mlp_new = update_matrix(mlp_param, mlp_grad, mlp_rows, mlp_cols)
    attn_new = update_matrix(attn_param, attn_grad, attn_rows, attn_cols)
    return (mlp_new, attn_new, mlp_rows, mlp_cols, attn_rows, attn_cols, attn_new.astype(jnp.bfloat16))
```

```python
import jax
import jax.numpy as jnp
from jax import lax
from jax.sharding import Mesh
from jax.sharding import PartitionSpec as P

STEP = 4
ROW = ("row_0", "row_1")
COL = ("col_0", "col_1", "col_2")
Y_HI, Z, CORE = COL
PLANE = (Y_HI, "row_0", "row_1")

TINY_SQUARE = 1e-30
LEARN_RATE = 0.05
DECAY_POWER = 0.8


def from_everyone(value, axes):
    length = lax.axis_size(axes)
    return lax.all_to_all(
        jnp.broadcast_to(value[None], (length, *value.shape)), axes, 0, 0, tiled=True
    )


def other_core(value):
    return lax.ppermute(value, CORE, [(0, 1), (1, 0)])


def local(
    mlp_param,
    mlp_grad,
    mlp_row_state,
    mlp_col_state,
    attn_param,
    attn_grad,
    attn_row_state,
    attn_col_state,
):
    keep = 1.0 - STEP ** (-DECAY_POWER)
    rows, mlp_cols = mlp_grad.shape
    attn_cols = attn_grad.shape[1]
    half = rows // 2
    row_devices = lax.axis_size(ROW)
    rows_total = rows * row_devices
    mlp_width = mlp_cols * lax.axis_size(COL)
    attn_width = attn_cols * lax.axis_size(COL)
    mlp_count = float(rows_total * mlp_width)
    attn_count = float(rows_total * attn_width)
    y_hi = lax.axis_index(Y_HI)
    row = lax.axis_index(ROW)
    core = lax.axis_index(CORE)
    attn_grad, attn_param = attn_grad.T, attn_param.T

    mlp_g2 = jnp.square(mlp_grad.astype(jnp.float32))
    attn_g2 = jnp.square(attn_grad.astype(jnp.float32))
    mlp_square, attn_square = mlp_g2 + TINY_SQUARE, attn_g2 + TINY_SQUARE
    row_sums = jnp.concatenate([jnp.sum(mlp_square, axis=1), jnp.sum(attn_square, axis=0)])
    col_sums = jnp.concatenate([jnp.sum(mlp_square, axis=0), jnp.sum(attn_square, axis=1)])
    col_sums = jnp.pad(col_sums, (0, 2 * rows - col_sums.size))
    p_mlp, p_attn = jnp.sum(jnp.square(mlp_param)), jnp.sum(jnp.square(attn_param))

    same = jnp.arange(2)[:, None, None] == y_hi
    sent = jnp.where(same, col_sums, row_sums)
    sent = jnp.broadcast_to(sent, (2, row_devices, 2 * rows)).reshape(2 * row_devices, 2 * rows)
    got = lax.all_to_all(sent, PLANE, 0, 0, tiled=True)
    place = jnp.arange(2 * row_devices)[:, None]
    col_total = jnp.sum(jnp.where(place // row_devices == y_hi, got, 0.0), axis=0)
    from_partner = place == (1 - y_hi) * row_devices + row
    row_sums = row_sums + jnp.sum(jnp.where(from_partner, got, 0.0), axis=0)
    mlp_cols_new = keep * mlp_col_state + (1.0 - keep) * (col_total[:mlp_cols] / rows_total)
    attn_cols_new = keep * attn_col_state + (1.0 - keep) * (
        col_total[mlp_cols : mlp_cols + attn_cols] / rows_total
    )

    w_mlp = jnp.sum(mlp_g2 * (1.0 / mlp_cols_new)[None, :], axis=1)
    w_attn = jnp.sum(attn_g2 * (1.0 / attn_cols_new)[:, None], axis=0)
    p_sums = jnp.pad(jnp.stack([p_mlp, p_attn]), (0, 126))
    packed = jnp.concatenate([row_sums, w_mlp, w_attn, p_sums])
    packed = packed + other_core(packed)
    mine = lax.dynamic_index_in_dim(packed[: 4 * rows].reshape(4, 2, half), core, 1, keepdims=False)
    mine = jnp.concatenate([mine.reshape(-1), packed[4 * rows :]])
    mine = from_everyone(mine, Z).sum(axis=0)
    r_mlp, r_attn, w_mlp, w_attn = mine[: 4 * half].reshape(4, half)
    p_mlp, p_attn = mine[4 * half], mine[4 * half + 1]
    mlp_state = lax.dynamic_index_in_dim(mlp_row_state.reshape(2, half), core, 0, keepdims=False)
    attn_state = lax.dynamic_index_in_dim(attn_row_state.reshape(2, half), core, 0, keepdims=False)
    mlp_half = keep * mlp_state + (1.0 - keep) * (r_mlp / mlp_width)
    attn_half = keep * attn_state + (1.0 - keep) * (r_attn / attn_width)
    q_sums = jnp.stack([jnp.sum(w_mlp / mlp_half), jnp.sum(w_attn / attn_half)])

    sent = jnp.concatenate([mlp_half, attn_half, jnp.pad(q_sums, (0, 126))])
    got = other_core(sent)
    first, last = jnp.where(core == 0, sent, got), jnp.where(core == 0, got, sent)
    mlp_rows_new = jnp.concatenate([first[:half], last[:half]])
    attn_rows_new = jnp.concatenate([first[half : 2 * half], last[half : 2 * half]])
    q_sums = q_sums + got[2 * half : 2 * half + 2]

    totals = jnp.concatenate([q_sums, jnp.stack([p_mlp, p_attn]), jnp.zeros((124,), jnp.float32)])
    totals = from_everyone(totals, PLANE).sum(axis=0)
    mlp_clip = jnp.maximum(1.0, jnp.sqrt(totals[0] / mlp_count))
    attn_clip = jnp.maximum(1.0, jnp.sqrt(totals[1] / attn_count))
    mlp_step = LEARN_RATE * jnp.sqrt(totals[2] / mlp_count)
    attn_step = LEARN_RATE * jnp.sqrt(totals[3] / attn_count)

    attn_scale = (attn_step / attn_clip) * lax.rsqrt(attn_cols_new)
    attn_new = attn_param - attn_grad.astype(jnp.float32) * attn_scale[:, None] * lax.rsqrt(attn_rows_new)[None, :]
    mlp_scale = (mlp_step / mlp_clip) * lax.rsqrt(mlp_rows_new)
    mlp_new = mlp_param - mlp_grad.astype(jnp.float32) * mlp_scale[:, None] * lax.rsqrt(mlp_cols_new)[None, :]
    block, mlp_new = lax.optimization_barrier((attn_new.astype(jnp.bfloat16), mlp_new))
    copy = from_everyone(block, ROW)
    copy = jnp.moveaxis(copy, 0, 1).reshape(attn_cols, rows_total).T
    return (
        mlp_new,
        attn_new.T,
        mlp_rows_new,
        mlp_cols_new,
        attn_rows_new,
        attn_cols_new,
        copy,
    )


def solution(mesh):
    finer = Mesh(mesh.devices.reshape(4, 2, 2, 8, 2), (*ROW, *COL))
    return jax.shard_map(
        local,
        mesh=finer,
        in_specs=(
            P(ROW, COL),
            P(ROW, COL),
            P(ROW),
            P(COL),
            P(ROW, COL),
            P(ROW, COL),
            P(ROW),
            P(COL),
        ),
        out_specs=(P(ROW, COL), P(ROW, COL), P(ROW), P(COL), P(ROW), P(COL), P(None, COL)),
        check_vma=False,
    )
```

```python
import functools

import jax
import jax.numpy as jnp
from jax import lax
from jax.experimental import pallas as pl
from jax.experimental.pallas import tpu as pltpu
from jax.sharding import Mesh
from jax.sharding import PartitionSpec as P

STEP = 4
ROW = ("row_0", "row_1")
COL = ("col_0", "col_1", "col_2")
Y_HI, Z, CORE = COL
PLANE = (Y_HI, "row_0", "row_1")

TINY_SQUARE = 1e-30
LEARN_RATE = 0.05
DECAY_POWER = 0.8
KEEP = 1.0 - STEP ** (-DECAY_POWER)

F32, BF16 = jnp.float32, jnp.bfloat16
SLAB = 16
LANES = 128
ON_CHIP = pl.BlockSpec(memory_space=pltpu.VMEM)
OFF_CHIP = pl.BlockSpec(memory_space=pltpu.HBM)


def call(kernel, outs, args, in_specs=None, out_specs=None, scratch=(), limit=4 << 20):
    return pl.pallas_call(
        kernel,
        out_shape=outs,
        in_specs=in_specs or [ON_CHIP] * len(args),
        out_specs=out_specs or [ON_CHIP] * len(outs),
        scratch_shapes=scratch,
        compiler_params=pltpu.CompilerParams(vmem_limit_bytes=limit),
    )(*args)


def tiles(value):
    width = value.shape[1] // LANES
    return sum((value[:, k * LANES : (k + 1) * LANES] for k in range(1, width)), value[:, :LANES])


def wide(value, width):
    return jnp.concatenate([value] * (width // LANES), axis=1)


def turned_sum(ref, start):
    return jnp.sum(ref[pl.ds(start, LANES), :].T, axis=0, keepdims=True)


def down(value):
    return jnp.broadcast_to(value, (LANES, LANES)).T


def fold(value):
    return value[:8] + value[8:]


def sums_kernel(
    g_hbm, ga_hbm, p_hbm, pa_hbm, sent_ref, rows_ref, psum_ref, g_ref, ga_ref, p_ref, pa_ref, lane_ref, acc_ref, sems
):
    rows, cols = g_hbm.shape
    attn_cols = ga_hbm.shape[0]
    blocks = rows // LANES
    g_copies = [
        pltpu.make_async_copy(g_hbm.at[pl.ds(b * LANES, LANES)], g_ref.at[pl.ds(b * LANES, LANES)], sems.at[b])
        for b in range(blocks)
    ]
    p_copies = [
        pltpu.make_async_copy(
            p_hbm.at[pl.ds(b * LANES, LANES)], p_ref.at[pl.ds(b * LANES, LANES)], sems.at[blocks + b]
        )
        for b in range(blocks)
    ]
    ga_copy = pltpu.make_async_copy(ga_hbm, ga_ref, sems.at[2 * blocks])
    pa_copy = pltpu.make_async_copy(pa_hbm, pa_ref, sems.at[2 * blocks + 1])
    for copy in (*g_copies, ga_copy, *p_copies, pa_copy):
        copy.start()
    acc_ref[...] = jnp.zeros_like(acc_ref)
    lane_ref[pl.ds(rows, 2 * LANES), :] = jnp.zeros((2 * LANES, LANES), F32)

    def squares(ref, start, first):
        def step(s, acc):
            g = ref[pl.ds(start + s * SLAB, SLAB), :].astype(F32)
            g = g * g
            lane_ref[pl.ds(first + start + s * SLAB, SLAB), :] = tiles(g)
            return acc + fold(g)

        return step

    def own_squares(ref, start):
        def step(s, acc):
            p = ref[pl.ds(start + s * SLAB, SLAB), :]
            return acc + fold(p * p)

        return step

    eight = jnp.zeros((8, cols), F32)
    steps = LANES // SLAB
    col_sum = eight
    for b, copy in enumerate(g_copies):
        copy.wait()
        col_sum = lax.fori_loop(0, steps, squares(g_ref, b * LANES, 0), col_sum, unroll=True)
        rows_ref[:, pl.ds(b * LANES, LANES)] = turned_sum(lane_ref, b * LANES)
    ga_copy.wait()
    row_sum = lax.fori_loop(0, attn_cols // SLAB, squares(ga_ref, 0, rows), jnp.zeros((8, rows), F32), unroll=4)
    rows_ref[:, pl.ds(rows, rows)] = jnp.sum(row_sum, axis=0, keepdims=True)
    rows_ref[...] += jnp.concatenate(
        [jnp.full((1, rows), cols * TINY_SQUARE, F32), jnp.full((1, rows), attn_cols * TINY_SQUARE, F32)], axis=1
    )
    col_sums = jnp.concatenate(
        [
            jnp.sum(col_sum, axis=0, keepdims=True),
            turned_sum(lane_ref, rows),
            turned_sum(lane_ref, rows + LANES),
        ],
        axis=1,
    ) + rows * TINY_SQUARE
    col_sums = jnp.concatenate([col_sums, jnp.zeros((1, 2 * rows - col_sums.shape[1]), F32)], axis=1)
    y_hi = lax.axis_index(Y_HI)
    devices = sent_ref.shape[0] // 2
    row_sums = rows_ref[...]
    for part in range(2):
        value = jnp.where(y_hi == part, col_sums, row_sums)
        for k in range(devices):
            sent_ref[part * devices + k] = value
    p_sum = eight
    for b, copy in enumerate(p_copies):
        copy.wait()
        p_sum = lax.fori_loop(0, steps, own_squares(p_ref, b * LANES), p_sum, unroll=True)
    pa_copy.wait()
    pa_sum = lax.fori_loop(0, attn_cols // SLAB, own_squares(pa_ref, 0), jnp.zeros((8, rows), F32), unroll=4)
    psum_ref[:, :LANES] = jnp.sum(tiles(p_sum), axis=0, keepdims=True)
    psum_ref[:, LANES:] = jnp.sum(tiles(pa_sum), axis=0, keepdims=True)


def columns_kernel(
    rows_total, got_ref, rows_ref, psum_ref, g_ref, ga_ref, state_ref, attn_state_ref,
    cols_ref, attn_cols_ref, kept_ref, sent_ref, lane_ref,
):
    rows, cols = g_ref.shape
    attn_cols = ga_ref.shape[0]
    half = rows // 2
    devices = got_ref.shape[0] // 2
    y_hi, core = lax.axis_index(Y_HI), lax.axis_index(CORE)
    row = lax.axis_index("row_0") * lax.axis_size("row_1") + lax.axis_index("row_1")
    total = got_ref[y_hi * devices]
    for k in range(1, devices):
        total = total + got_ref[y_hi * devices + k]
    row_sums = rows_ref[...] + got_ref[(1 - y_hi) * devices + row]
    cols_new = KEEP * state_ref[...].reshape(1, cols) + (1.0 - KEEP) * (total[:, :cols] / rows_total)
    cols_ref[...] = cols_new.reshape(cols)
    attn_state = attn_state_ref[...].reshape(1, attn_cols)
    attn_new = KEEP * attn_state + (1.0 - KEEP) * (total[:, cols : cols + attn_cols] / rows_total)
    attn_cols_ref[...] = attn_new.reshape(attn_cols)
    inverse = jnp.broadcast_to(1.0 / cols_new, (SLAB, cols))
    attn_inverse = jnp.concatenate([1.0 / attn_new, jnp.ones((1, 2 * LANES - attn_cols), F32)], axis=1)
    down_inverse = [down(attn_inverse[:, k * LANES : (k + 1) * LANES]) for k in range(2)]

    def step(s, carry):
        g = g_ref[pl.ds(s * SLAB, SLAB), :].astype(F32)
        lane_ref[pl.ds(s * SLAB, SLAB), :] = tiles(g * g * inverse)
        return carry

    lax.fori_loop(0, rows // SLAB, step, 0, unroll=8)
    w_attn = jnp.zeros((8, rows), F32)
    for s in range(attn_cols // SLAB):
        g = ga_ref[pl.ds(s * SLAB, SLAB), :].astype(F32)
        at = s * SLAB
        scale = down_inverse[at // LANES][at % LANES : at % LANES + SLAB]
        w_attn = w_attn + fold(g * g * wide(scale, rows))
    w_attn = jnp.sum(w_attn, axis=0, keepdims=True)
    w_mlp = jnp.concatenate([turned_sum(lane_ref, b * LANES) for b in range(rows // LANES)], axis=1)
    p_sums = psum_ref[...]
    vectors = (row_sums[:, :rows], row_sums[:, rows:], w_mlp, w_attn)
    first = jnp.concatenate([v[:, :half] for v in vectors] + [p_sums], axis=1)
    last = jnp.concatenate([v[:, half:] for v in vectors] + [p_sums], axis=1)
    kept_ref[...] = jnp.where(core == 0, first, last)
    sent_ref[...] = jnp.where(core == 0, last, first)


def spread_kernel(kept_ref, got_ref, sent_ref):
    value = kept_ref[...] + got_ref[...]
    for k in range(sent_ref.shape[0]):
        sent_ref[k] = value


def rows_kernel(widths, got_ref, state_ref, attn_state_ref, sent_ref, psum_ref):
    rows = state_ref.shape[0]
    half = rows // 2
    core = lax.axis_index(CORE)
    total = got_ref[0]
    for k in range(1, got_ref.shape[0]):
        total = total + got_ref[k]
    psum_ref[...] = total[:, 4 * half :]
    for k, (ref, width) in enumerate(zip((state_ref, attn_state_ref), widths)):
        state = ref[...].reshape(1, rows)
        state = jnp.where(core == 0, state[:, :half], state[:, half:])
        new = KEEP * state + (1.0 - KEEP) * (total[:, k * half : (k + 1) * half] / width)
        sent_ref[:, k * half : (k + 1) * half] = new
        part = total[:, (2 + k) * half : (3 + k) * half] / new
        sent_ref[:, 2 * half + k * LANES : 2 * half + (k + 1) * LANES] = tiles(part)


def scalars_kernel(own_ref, got_ref, psum_ref, rows_ref, attn_rows_ref, sent_ref):
    rows = rows_ref.shape[0]
    half = rows // 2
    core = lax.axis_index(CORE)
    own, got = own_ref[...], got_ref[...]
    first, last = jnp.where(core == 0, own, got), jnp.where(core == 0, got, own)
    rows_ref[...] = jnp.concatenate([first[:, :half], last[:, :half]], axis=1).reshape(rows)
    attn_rows_ref[...] = jnp.concatenate([first[:, half : 2 * half], last[:, half : 2 * half]], axis=1).reshape(rows)
    value = jnp.concatenate([first[:, 2 * half :] + last[:, 2 * half :], psum_ref[...]], axis=1)
    for k in range(sent_ref.shape[0]):
        sent_ref[k] = value


def update_kernel(
    counts, got_ref, rows_ref, attn_rows_ref, cols_ref, attn_cols_ref, g_ref, ga_ref, p_ref, pa_ref,
    new_hbm, attn_hbm, rows_hbm, cols_hbm, attn_rows_hbm, attn_cols_hbm, block_ref, new_ref, attn_ref, sems,
):
    rows, cols = g_ref.shape
    attn_cols = ga_ref.shape[0]
    blocks = rows // LANES
    pairs = ((rows_ref, rows_hbm), (cols_ref, cols_hbm), (attn_rows_ref, attn_rows_hbm), (attn_cols_ref, attn_cols_hbm))
    copies = [pltpu.make_async_copy(a, b, sems.at[blocks + 1 + k]) for k, (a, b) in enumerate(pairs)]
    for copy in copies:
        copy.start()
    total = got_ref[0]
    for k in range(1, got_ref.shape[0]):
        total = total + got_ref[k]
    q_mlp, q_attn, p_mlp, p_attn = (
        jnp.sum(total[:, k * LANES : (k + 1) * LANES], axis=1, keepdims=True) for k in range(4)
    )

    def factor(q, p, count):
        clip = jnp.maximum(1.0, jnp.sqrt(jnp.broadcast_to(q, (1, LANES)) / count))
        return LEARN_RATE * jnp.sqrt(jnp.broadcast_to(p, (1, LANES)) / count) / clip

    mlp_factor, attn_factor = factor(q_mlp, p_mlp, counts[0]), factor(q_attn, p_attn, counts[1])
    along = jnp.broadcast_to(lax.rsqrt(attn_rows_ref[...].reshape(1, rows)), (SLAB, rows))
    across = lax.rsqrt(jnp.concatenate([attn_cols_ref[...].reshape(1, attn_cols), jnp.ones((1, 2 * LANES - attn_cols), F32)], axis=1))
    across = [down(across[:, k * LANES : (k + 1) * LANES] * attn_factor) for k in range(2)]
    for s in range(attn_cols // SLAB):
        at = s * SLAB
        scale = across[at // LANES][at % LANES : at % LANES + SLAB]
        new = pa_ref[pl.ds(at, SLAB), :] - ga_ref[pl.ds(at, SLAB), :].astype(F32) * wide(scale, rows) * along
        attn_ref[pl.ds(at, SLAB), :] = new
        new = new.astype(BF16)
        for k in range(block_ref.shape[0]):
            block_ref[k, pl.ds(at, SLAB), :] = new
    attn_copy = pltpu.make_async_copy(attn_ref, attn_hbm, sems.at[blocks])
    attn_copy.start()
    along = jnp.broadcast_to(lax.rsqrt(cols_ref[...].reshape(1, cols)), (SLAB, cols))
    row_scale = lax.rsqrt(rows_ref[...].reshape(1, rows))
    for b in range(blocks):
        across = down(row_scale[:, b * LANES : (b + 1) * LANES] * mlp_factor)
        for s in range(LANES // SLAB):
            at = pl.ds(b * LANES + s * SLAB, SLAB)
            scale = across[s * SLAB : (s + 1) * SLAB]
            new_ref[at, :] = p_ref[at, :] - g_ref[at, :].astype(F32) * wide(scale, cols) * along
        at = pl.ds(b * LANES, LANES)
        copies.append(pltpu.make_async_copy(new_ref.at[at], new_hbm.at[at], sems.at[b]))
        copies[-1].start()
    for copy in (attn_copy, *copies):
        copy.wait()


def assemble_kernel(got_ref, out_hbm, sems):
    rows = got_ref.shape[2]
    copies = [
        pltpu.make_async_copy(got_ref.at[k], out_hbm.at[:, pl.ds(k * rows, rows)], sems.at[k])
        for k in range(got_ref.shape[0])
    ]
    for copy in copies:
        copy.start()
    for copy in copies:
        copy.wait()


def everyone(value, axes):
    return lax.all_to_all(value, axes, 0, 0, tiled=True)


def other_core(value):
    return lax.ppermute(value, CORE, [(0, 1), (1, 0)])


def local(
    mlp_param,
    mlp_grad,
    mlp_row_state,
    mlp_col_state,
    attn_param,
    attn_grad,
    attn_row_state,
    attn_col_state,
):
    rows, cols = mlp_grad.shape
    attn_cols = attn_grad.shape[1]
    half = rows // 2
    row_devices, plane, layers = lax.axis_size(ROW), lax.axis_size(PLANE), lax.axis_size(Z)
    rows_total = rows * row_devices
    widths = (float(cols * lax.axis_size(COL)), float(attn_cols * lax.axis_size(COL)))
    counts = (rows_total * widths[0], rows_total * widths[1])
    attn_grad, attn_param = attn_grad.T, attn_param.T
    blocks = rows // LANES

    sent, row_sums, p_sums, g, ga, p, pa = call(
        sums_kernel,
        [
            pltpu.VMEM((plane, 1, 2 * rows), F32),
            pltpu.VMEM((1, 2 * rows), F32),
            pltpu.VMEM((1, 2 * LANES), F32),
            pltpu.VMEM((rows, cols), BF16),
            pltpu.VMEM((attn_cols, rows), BF16),
            pltpu.VMEM((rows, cols), F32),
            pltpu.VMEM((attn_cols, rows), F32),
        ],
        (mlp_grad, attn_grad, mlp_param, attn_param),
        in_specs=[OFF_CHIP] * 4,
        scratch=[
            pltpu.VMEM((rows + 2 * LANES, LANES), F32),
            pltpu.VMEM((8, LANES), F32),
            pltpu.SemaphoreType.DMA((2 * blocks + 2,)),
        ],
        limit=119 << 19,
    )
    got = everyone(sent, PLANE)
    cols_new, attn_cols_new, kept, sent = call(
        functools.partial(columns_kernel, float(rows_total)),
        [
            pltpu.VMEM((cols,), F32),
            pltpu.VMEM((attn_cols,), F32),
            pltpu.VMEM((1, 4 * half + 2 * LANES), F32),
            pltpu.VMEM((1, 4 * half + 2 * LANES), F32),
        ],
        (got, row_sums, p_sums, g, ga, mlp_col_state, attn_col_state),
        scratch=[pltpu.VMEM((rows, LANES), F32)],
    )
    (sent,) = call(
        spread_kernel,
        [pltpu.VMEM((layers, 1, 4 * half + 2 * LANES), F32)],
        (kept, other_core(sent)),
    )
    sent, p_sums = call(
        functools.partial(rows_kernel, widths),
        [pltpu.VMEM((1, 2 * half + 2 * LANES), F32), pltpu.VMEM((1, 2 * LANES), F32)],
        (everyone(sent, Z), mlp_row_state, attn_row_state),
    )
    rows_new, attn_rows_new, sent = call(
        scalars_kernel,
        [
            pltpu.VMEM((rows,), F32),
            pltpu.VMEM((rows,), F32),
            pltpu.VMEM((plane, 1, 4 * LANES), F32),
        ],
        (sent, other_core(sent), p_sums),
    )
    mlp_new, attn_new, rows_out, cols_out, attn_rows_out, attn_cols_out, block = call(
        functools.partial(update_kernel, counts),
        [
            jax.ShapeDtypeStruct((rows, cols), F32),
            jax.ShapeDtypeStruct((attn_cols, rows), F32),
            jax.ShapeDtypeStruct((rows,), F32),
            jax.ShapeDtypeStruct((cols,), F32),
            jax.ShapeDtypeStruct((rows,), F32),
            jax.ShapeDtypeStruct((attn_cols,), F32),
            pltpu.VMEM((row_devices, attn_cols, rows), BF16),
        ],
        (everyone(sent, PLANE), rows_new, attn_rows_new, cols_new, attn_cols_new, g, ga, p, pa),
        out_specs=[OFF_CHIP] * 6 + [ON_CHIP],
        scratch=[
            pltpu.VMEM((rows, cols), F32),
            pltpu.VMEM((attn_cols, rows), F32),
            pltpu.SemaphoreType.DMA((blocks + 5,)),
        ],
        limit=16 << 20,
    )
    (copy,) = call(
        assemble_kernel,
        [jax.ShapeDtypeStruct((attn_cols, rows_total), BF16)],
        (everyone(block, ROW),),
        out_specs=[OFF_CHIP],
        scratch=[pltpu.SemaphoreType.DMA((row_devices,))],
    )
    return (
        mlp_new,
        attn_new.T,
        rows_out,
        cols_out,
        attn_rows_out,
        attn_cols_out,
        copy.T,
    )


def solution(mesh):
    finer = Mesh(mesh.devices.reshape(4, 2, 2, 8, 2), (*ROW, *COL))
    return jax.shard_map(
        local,
        mesh=finer,
        in_specs=(
            P(ROW, COL),
            P(ROW, COL),
            P(ROW),
            P(COL),
            P(ROW, COL),
            P(ROW, COL),
            P(ROW),
            P(COL),
        ),
        out_specs=(P(ROW, COL), P(ROW, COL), P(ROW), P(COL), P(ROW), P(COL), P(None, COL)),
        check_vma=False,
    )
```

```python
import functools

import jax
import jax.numpy as jnp
from jax import lax
from jax.experimental import pallas as pl
from jax.experimental.pallas import tpu as pltpu
from jax.sharding import Mesh
from jax.sharding import PartitionSpec as P

STEP = 4
ROW = ("row_0", "row_1")
COL = ("col_0", "col_1", "col_2")
Y_HI, Z, CORE = COL
LAYERS = (Y_HI, Z)

TINY_SQUARE = 1e-30
LEARN_RATE = 0.05
DECAY_POWER = 0.8
KEEP = 1.0 - STEP ** (-DECAY_POWER)

F32, BF16 = jnp.float32, jnp.bfloat16
SLAB = 16
LANES = 128
ON_CHIP = pl.BlockSpec(memory_space=pltpu.VMEM)
OFF_CHIP = pl.BlockSpec(memory_space=pltpu.HBM)


def call(kernel, outs, args, in_specs=None, out_specs=None, scratch=(), limit=4 << 20):
    return pl.pallas_call(
        kernel,
        out_shape=outs,
        in_specs=in_specs or [ON_CHIP] * len(args),
        out_specs=out_specs or [ON_CHIP] * len(outs),
        scratch_shapes=scratch,
        compiler_params=pltpu.CompilerParams(vmem_limit_bytes=limit),
    )(*args)


def tiles(value):
    width = value.shape[1] // LANES
    return sum((value[:, k * LANES : (k + 1) * LANES] for k in range(1, width)), value[:, :LANES])


def wide(value, width):
    return jnp.concatenate([value] * (width // LANES), axis=1)


def turned_sum(ref, start):
    return jnp.sum(ref[pl.ds(start, LANES), :].T, axis=0, keepdims=True)


def down(value):
    return jnp.broadcast_to(value, (LANES, LANES)).T


def fold(value):
    return value[:8] + value[8:]


def added(ref):
    total = ref[0]
    for k in range(1, ref.shape[0]):
        total = total + ref[k]
    return total


def sums_kernel(
    g_hbm, ga_hbm, p_hbm, pa_hbm, sent_ref, rows_ref, psum_ref, g_ref, ga_ref, p_ref, pa_ref, lane_ref, sems
):
    rows, cols = g_hbm.shape
    attn_cols = ga_hbm.shape[0]
    blocks = rows // LANES
    g_copies = [
        pltpu.make_async_copy(g_hbm.at[pl.ds(b * LANES, LANES)], g_ref.at[pl.ds(b * LANES, LANES)], sems.at[b])
        for b in range(blocks)
    ]
    p_copies = [
        pltpu.make_async_copy(
            p_hbm.at[pl.ds(b * LANES, LANES)], p_ref.at[pl.ds(b * LANES, LANES)], sems.at[blocks + b]
        )
        for b in range(blocks)
    ]
    ga_copy = pltpu.make_async_copy(ga_hbm, ga_ref, sems.at[2 * blocks])
    pa_copy = pltpu.make_async_copy(pa_hbm, pa_ref, sems.at[2 * blocks + 1])
    for copy in (*g_copies, ga_copy, *p_copies, pa_copy):
        copy.start()
    lane_ref[pl.ds(rows, 2 * LANES), :] = jnp.zeros((2 * LANES, LANES), F32)

    def squares(ref, start, first):
        def step(s, acc):
            g = ref[pl.ds(start + s * SLAB, SLAB), :].astype(F32)
            g = g * g
            lane_ref[pl.ds(first + start + s * SLAB, SLAB), :] = tiles(g)
            return acc + fold(g)

        return step

    def own_squares(ref, start):
        def step(s, acc):
            p = ref[pl.ds(start + s * SLAB, SLAB), :]
            return acc + fold(p * p)

        return step

    eight = jnp.zeros((8, cols), F32)
    steps = LANES // SLAB
    col_sum = eight
    for b, copy in enumerate(g_copies):
        copy.wait()
        col_sum = lax.fori_loop(0, steps, squares(g_ref, b * LANES, 0), col_sum, unroll=True)
        rows_ref[:, pl.ds(b * LANES, LANES)] = turned_sum(lane_ref, b * LANES)
    ga_copy.wait()
    row_sum = lax.fori_loop(0, attn_cols // SLAB, squares(ga_ref, 0, rows), jnp.zeros((8, rows), F32), unroll=4)
    rows_ref[:, pl.ds(rows, rows)] = jnp.sum(row_sum, axis=0, keepdims=True)
    rows_ref[...] += jnp.concatenate(
        [jnp.full((1, rows), cols * TINY_SQUARE, F32), jnp.full((1, rows), attn_cols * TINY_SQUARE, F32)], axis=1
    )
    col_sums = jnp.concatenate(
        [
            jnp.sum(col_sum, axis=0, keepdims=True),
            turned_sum(lane_ref, rows),
            turned_sum(lane_ref, rows + LANES),
        ],
        axis=1,
    ) + rows * TINY_SQUARE
    for k in range(sent_ref.shape[0]):
        sent_ref[k] = col_sums
    p_sum = eight
    for b, copy in enumerate(p_copies):
        copy.wait()
        p_sum = lax.fori_loop(0, steps, own_squares(p_ref, b * LANES), p_sum, unroll=True)
    pa_copy.wait()
    pa_sum = lax.fori_loop(0, attn_cols // SLAB, own_squares(pa_ref, 0), jnp.zeros((8, rows), F32), unroll=4)
    psum_ref[:, :LANES] = jnp.sum(tiles(p_sum), axis=0, keepdims=True)
    psum_ref[:, LANES:] = jnp.sum(tiles(pa_sum), axis=0, keepdims=True)


def columns_kernel(
    rows_total, got_ref, rows_ref, g_ref, ga_ref, state_ref, attn_state_ref,
    cols_ref, attn_cols_ref, kept_ref, sent_ref, lane_ref,
):
    rows, cols = g_ref.shape
    attn_cols = ga_ref.shape[0]
    half = rows // 2
    core = lax.axis_index(CORE)
    total = added(got_ref)
    row_sums = rows_ref[...]
    cols_new = KEEP * state_ref[...].reshape(1, cols) + (1.0 - KEEP) * (total[:, :cols] / rows_total)
    cols_ref[...] = cols_new.reshape(cols)
    attn_state = attn_state_ref[...].reshape(1, attn_cols)
    attn_new = KEEP * attn_state + (1.0 - KEEP) * (total[:, cols : cols + attn_cols] / rows_total)
    attn_cols_ref[...] = attn_new.reshape(attn_cols)
    inverse = jnp.broadcast_to(1.0 / cols_new, (SLAB, cols))
    attn_inverse = jnp.concatenate([1.0 / attn_new, jnp.ones((1, 2 * LANES - attn_cols), F32)], axis=1)
    down_inverse = [down(attn_inverse[:, k * LANES : (k + 1) * LANES]) for k in range(2)]

    def step(s, carry):
        g = g_ref[pl.ds(s * SLAB, SLAB), :].astype(F32)
        lane_ref[pl.ds(s * SLAB, SLAB), :] = tiles(g * g * inverse)
        return carry

    lax.fori_loop(0, rows // SLAB, step, 0, unroll=8)
    w_attn = jnp.zeros((8, rows), F32)
    for s in range(attn_cols // SLAB):
        g = ga_ref[pl.ds(s * SLAB, SLAB), :].astype(F32)
        at = s * SLAB
        scale = down_inverse[at // LANES][at % LANES : at % LANES + SLAB]
        w_attn = w_attn + fold(g * g * wide(scale, rows))
    w_attn = jnp.sum(w_attn, axis=0, keepdims=True)
    w_mlp = jnp.concatenate([turned_sum(lane_ref, b * LANES) for b in range(rows // LANES)], axis=1)
    vectors = (row_sums[:, :rows], row_sums[:, rows:], w_mlp, w_attn)
    first = jnp.concatenate([v[:, :half] for v in vectors], axis=1)
    last = jnp.concatenate([v[:, half:] for v in vectors], axis=1)
    kept_ref[...] = jnp.where(core == 0, first, last)
    sent_ref[...] = jnp.where(core == 0, last, first)


def spread_kernel(kept_ref, got_ref, psum_ref, sent_ref):
    value = jnp.concatenate([kept_ref[...] + got_ref[...], psum_ref[...]], axis=1)
    for k in range(sent_ref.shape[0]):
        sent_ref[k] = value


def rows_kernel(widths, got_ref, state_ref, attn_state_ref, sent_ref):
    rows = state_ref.shape[0]
    half = rows // 2
    core = lax.axis_index(CORE)
    total = added(got_ref)
    new, parts = [], []
    for k, (ref, width) in enumerate(zip((state_ref, attn_state_ref), widths)):
        state = ref[...].reshape(1, rows)
        state = jnp.where(core == 0, state[:, :half], state[:, half:])
        new.append(KEEP * state + (1.0 - KEEP) * (total[:, k * half : (k + 1) * half] / width))
        parts.append(tiles(total[:, (2 + k) * half : (3 + k) * half] / new[k]))
    value = jnp.concatenate([*parts, total[:, 4 * half :], *new], axis=1)
    for k in range(sent_ref.shape[0]):
        sent_ref[k] = value


def factor(got_ref, matrix, count):
    total = got_ref[0, :, : 4 * LANES]
    for k in range(1, got_ref.shape[0]):
        total = total + got_ref[k, :, : 4 * LANES]
    q, p = (
        jnp.broadcast_to(jnp.sum(total[:, k * LANES : (k + 1) * LANES], axis=1, keepdims=True), (1, LANES))
        for k in (matrix, 2 + matrix)
    )
    return LEARN_RATE * jnp.sqrt(p / count) / jnp.maximum(1.0, jnp.sqrt(q / count))


def new_rows(got_ref, matrix, half):
    row = lax.axis_index("row_0") * lax.axis_size("row_1") + lax.axis_index("row_1")
    at = pl.ds(4 * LANES + matrix * half, half)
    return jnp.concatenate([got_ref[2 * row, :, at], got_ref[2 * row + 1, :, at]], axis=1)


def attn_kernel(count, got_ref, attn_cols_ref, ga_ref, pa_ref, attn_ref, block_ref):
    attn_cols, rows = ga_ref.shape
    along = jnp.broadcast_to(lax.rsqrt(new_rows(got_ref, 1, rows // 2)), (SLAB, rows))
    across = attn_cols_ref[...].reshape(1, attn_cols)
    across = lax.rsqrt(jnp.concatenate([across, jnp.ones((1, 2 * LANES - attn_cols), F32)], axis=1))
    scale = factor(got_ref, 1, count)
    across = [down(across[:, k * LANES : (k + 1) * LANES] * scale) for k in range(2)]
    for s in range(attn_cols // SLAB):
        at = s * SLAB
        scale = across[at // LANES][at % LANES : at % LANES + SLAB]
        new = pa_ref[pl.ds(at, SLAB), :] - ga_ref[pl.ds(at, SLAB), :].astype(F32) * wide(scale, rows) * along
        attn_ref[pl.ds(at, SLAB), :] = new
        new = new.astype(BF16)
        for k in range(block_ref.shape[0]):
            block_ref[k, pl.ds(at, SLAB), :] = new


def finish_kernel(
    count, copy_ref, got_ref, cols_ref, attn_cols_ref, attn_ref, g_ref, p_ref,
    copy_hbm, attn_hbm, new_hbm, rows_hbm, cols_hbm, attn_rows_hbm, attn_cols_hbm,
    new_ref, rows_ref, attn_rows_ref, sems,
):
    rows, cols = g_ref.shape
    blocks = rows // LANES
    copies = []

    def put(source, target):
        copies.append(pltpu.make_async_copy(source, target, sems.at[len(copies)]))
        copies[-1].start()

    for k in range(copy_ref.shape[0]):
        put(copy_ref.at[k], copy_hbm.at[:, pl.ds(k * rows, rows)])
    put(attn_ref, attn_hbm)
    put(cols_ref, cols_hbm)
    put(attn_cols_ref, attn_cols_hbm)
    row_factors = new_rows(got_ref, 0, rows // 2)
    rows_ref[...] = row_factors.reshape(rows)
    attn_rows_ref[...] = new_rows(got_ref, 1, rows // 2).reshape(rows)
    along = jnp.broadcast_to(lax.rsqrt(cols_ref[...].reshape(1, cols)), (SLAB, cols))
    scale = factor(got_ref, 0, count)
    row_scale = lax.rsqrt(row_factors)
    for b in range(blocks):
        across = down(row_scale[:, b * LANES : (b + 1) * LANES] * scale)
        for s in range(LANES // SLAB):
            at = pl.ds(b * LANES + s * SLAB, SLAB)
            new_ref[at, :] = (
                p_ref[at, :] - g_ref[at, :].astype(F32) * wide(across[s * SLAB : (s + 1) * SLAB], cols) * along
            )
        at = pl.ds(b * LANES, LANES)
        put(new_ref.at[at], new_hbm.at[at])
    put(rows_ref, rows_hbm)
    put(attn_rows_ref, attn_rows_hbm)
    for copy in copies:
        copy.wait()


def everyone(value, axes):
    return lax.all_to_all(value, axes, 0, 0, tiled=True)


def other_core(value):
    return lax.ppermute(value, CORE, [(0, 1), (1, 0)])


def local(
    mlp_param,
    mlp_grad,
    mlp_row_state,
    mlp_col_state,
    attn_param,
    attn_grad,
    attn_row_state,
    attn_col_state,
):
    rows, cols = mlp_grad.shape
    attn_cols = attn_grad.shape[1]
    half = rows // 2
    row_devices, layers = lax.axis_size(ROW), lax.axis_size(LAYERS)
    message = -(-(cols + attn_cols) // LANES) * LANES
    rows_total = rows * row_devices
    widths = (float(cols * lax.axis_size(COL)), float(attn_cols * lax.axis_size(COL)))
    counts = (rows_total * widths[0], rows_total * widths[1])
    attn_grad, attn_param = attn_grad.T, attn_param.T
    blocks = rows // LANES

    sent, row_sums, p_sums, g, ga, p, pa = call(
        sums_kernel,
        [
            pltpu.VMEM((row_devices, 1, message), F32),
            pltpu.VMEM((1, 2 * rows), F32),
            pltpu.VMEM((1, 2 * LANES), F32),
            pltpu.VMEM((rows, cols), BF16),
            pltpu.VMEM((attn_cols, rows), BF16),
            pltpu.VMEM((rows, cols), F32),
            pltpu.VMEM((attn_cols, rows), F32),
        ],
        (mlp_grad, attn_grad, mlp_param, attn_param),
        in_specs=[OFF_CHIP] * 4,
        scratch=[
            pltpu.VMEM((rows + 2 * LANES, LANES), F32),
            pltpu.SemaphoreType.DMA((2 * blocks + 2,)),
        ],
        limit=119 << 19,
    )
    got = everyone(sent, ROW)
    cols_new, attn_cols_new, kept, sent = call(
        functools.partial(columns_kernel, float(rows_total)),
        [
            pltpu.VMEM((cols,), F32),
            pltpu.VMEM((attn_cols,), F32),
            pltpu.VMEM((1, 4 * half), F32),
            pltpu.VMEM((1, 4 * half), F32),
        ],
        (got, row_sums, g, ga, mlp_col_state, attn_col_state),
        scratch=[pltpu.VMEM((rows, LANES), F32)],
    )
    (sent,) = call(
        spread_kernel,
        [pltpu.VMEM((layers, 1, 4 * half + 2 * LANES), F32)],
        (kept, other_core(sent), p_sums),
    )
    (sent,) = call(
        functools.partial(rows_kernel, widths),
        [pltpu.VMEM((2 * row_devices, 1, 4 * LANES + 2 * half), F32)],
        (everyone(sent, LAYERS), mlp_row_state, attn_row_state),
    )
    got = everyone(sent, (*ROW, CORE))
    attn_new, block = call(
        functools.partial(attn_kernel, counts[1]),
        [pltpu.VMEM((attn_cols, rows), F32), pltpu.VMEM((row_devices, attn_cols, rows), BF16)],
        (got, attn_cols_new, ga, pa),
    )
    copy, attn_new, mlp_new, rows_new, cols_new, attn_rows_new, attn_cols_new = call(
        functools.partial(finish_kernel, counts[0]),
        [
            jax.ShapeDtypeStruct((attn_cols, rows_total), BF16),
            jax.ShapeDtypeStruct((attn_cols, rows), F32),
            jax.ShapeDtypeStruct((rows, cols), F32),
            jax.ShapeDtypeStruct((rows,), F32),
            jax.ShapeDtypeStruct((cols,), F32),
            jax.ShapeDtypeStruct((rows,), F32),
            jax.ShapeDtypeStruct((attn_cols,), F32),
        ],
        (everyone(block, ROW), got, cols_new, attn_cols_new, attn_new, g, p),
        out_specs=[OFF_CHIP] * 7,
        scratch=[
            pltpu.VMEM((rows, cols), F32),
            pltpu.VMEM((rows,), F32),
            pltpu.VMEM((rows,), F32),
            pltpu.SemaphoreType.DMA((row_devices + blocks + 5,)),
        ],
    )
    return mlp_new, attn_new.T, rows_new, cols_new, attn_rows_new, attn_cols_new, copy.T


def solution(mesh):
    finer = Mesh(mesh.devices.reshape(4, 2, 2, 8, 2), (*ROW, *COL))
    return jax.shard_map(
        local,
        mesh=finer,
        in_specs=(
            P(ROW, COL),
            P(ROW, COL),
            P(ROW),
            P(COL),
            P(ROW, COL),
            P(ROW, COL),
            P(ROW),
            P(COL),
        ),
        out_specs=(P(ROW, COL), P(ROW, COL), P(ROW), P(COL), P(ROW), P(COL), P(None, COL)),
        check_vma=False,
    )
```

```python
import functools

import jax
import jax.numpy as jnp
from jax import lax
from jax.experimental import pallas as pl
from jax.experimental.pallas import tpu as pltpu
from jax.sharding import Mesh
from jax.sharding import PartitionSpec as P

STEP = 4
ROW = ("row_0", "row_1")
COL = ("col_0", "col_1", "col_2")
Y_HI, Z, CORE = COL
LAYERS = (Y_HI, Z)

TINY_SQUARE = 1e-30
LEARN_RATE = 0.05
DECAY_POWER = 0.8
KEEP = 1.0 - STEP ** (-DECAY_POWER)

F32, BF16 = jnp.float32, jnp.bfloat16
SLAB = 16
LANES = 128
ON_CHIP = pl.BlockSpec(memory_space=pltpu.VMEM)
OFF_CHIP = pl.BlockSpec(memory_space=pltpu.HBM)


def call(kernel, outs, args, in_specs=None, out_specs=None, scratch=(), limit=4 << 20, aliases=None, flops=0):
    return pl.pallas_call(
        kernel,
        out_shape=outs,
        in_specs=in_specs or [ON_CHIP] * len(args),
        out_specs=out_specs or [ON_CHIP] * len(outs),
        scratch_shapes=scratch,
        input_output_aliases=aliases or {},
        cost_estimate=pl.CostEstimate(flops=flops, bytes_accessed=flops, transcendentals=0) if flops else None,
        compiler_params=pltpu.CompilerParams(vmem_limit_bytes=limit),
    )(*args)


def tiles(value):
    width = value.shape[1] // LANES
    return sum((value[:, k * LANES : (k + 1) * LANES] for k in range(1, width)), value[:, :LANES])


def wide(value, width):
    return jnp.concatenate([value] * (width // LANES), axis=1)


def turned_sum(ref, start):
    return jnp.sum(ref[pl.ds(start, LANES), :].T, axis=0, keepdims=True)


def down(value):
    return jnp.broadcast_to(value, (LANES, LANES)).T


def fold(value):
    return value[:8] + value[8:]


def added(ref):
    total = ref[0]
    for k in range(1, ref.shape[0]):
        total = total + ref[k]
    return total


def sums_kernel(
    g_hbm, ga_hbm, p_hbm, pa_hbm, sent_ref, rows_ref, psum_ref, g_ref, ga_ref, p_ref, pa_ref, lane_ref, sems
):
    rows, cols = g_hbm.shape
    attn_cols = ga_hbm.shape[0]
    blocks = rows // LANES
    g_copies = [
        pltpu.make_async_copy(g_hbm.at[pl.ds(b * LANES, LANES)], g_ref.at[pl.ds(b * LANES, LANES)], sems.at[b])
        for b in range(blocks)
    ]
    p_copies = [
        pltpu.make_async_copy(
            p_hbm.at[pl.ds(b * LANES, LANES)], p_ref.at[pl.ds(b * LANES, LANES)], sems.at[blocks + b]
        )
        for b in range(blocks)
    ]
    ga_copy = pltpu.make_async_copy(ga_hbm, ga_ref, sems.at[2 * blocks])
    pa_copy = pltpu.make_async_copy(pa_hbm, pa_ref, sems.at[2 * blocks + 1])
    for copy in (*g_copies, ga_copy, *p_copies, pa_copy):
        copy.start()
    lane_ref[pl.ds(rows, 2 * LANES), :] = jnp.zeros((2 * LANES, LANES), F32)

    def squares(ref, start, first):
        def step(s, acc):
            g = ref[pl.ds(start + s * SLAB, SLAB), :].astype(F32)
            g = g * g
            lane_ref[pl.ds(first + start + s * SLAB, SLAB), :] = tiles(g)
            return acc + fold(g)

        return step

    def own_squares(ref, start):
        def step(s, acc):
            p = ref[pl.ds(start + s * SLAB, SLAB), :]
            return acc + fold(p * p)

        return step

    eight = jnp.zeros((8, cols), F32)
    steps = LANES // SLAB
    col_sum = eight
    for b, copy in enumerate(g_copies):
        copy.wait()
        col_sum = lax.fori_loop(0, steps, squares(g_ref, b * LANES, 0), col_sum, unroll=True)
        rows_ref[:, pl.ds(b * LANES, LANES)] = turned_sum(lane_ref, b * LANES)
    ga_copy.wait()
    row_sum = lax.fori_loop(0, attn_cols // SLAB, squares(ga_ref, 0, rows), jnp.zeros((8, rows), F32), unroll=4)
    rows_ref[:, pl.ds(rows, rows)] = jnp.sum(row_sum, axis=0, keepdims=True)
    rows_ref[...] += jnp.concatenate(
        [jnp.full((1, rows), cols * TINY_SQUARE, F32), jnp.full((1, rows), attn_cols * TINY_SQUARE, F32)], axis=1
    )
    col_sums = jnp.concatenate(
        [
            jnp.sum(col_sum, axis=0, keepdims=True),
            turned_sum(lane_ref, rows),
            turned_sum(lane_ref, rows + LANES),
        ],
        axis=1,
    ) + rows * TINY_SQUARE
    for k in range(sent_ref.shape[0]):
        sent_ref[k] = col_sums
    p_sum = eight
    for b, copy in enumerate(p_copies):
        copy.wait()
        p_sum = lax.fori_loop(0, steps, own_squares(p_ref, b * LANES), p_sum, unroll=True)
    pa_copy.wait()
    pa_sum = lax.fori_loop(0, attn_cols // SLAB, own_squares(pa_ref, 0), jnp.zeros((8, rows), F32), unroll=4)
    psum_ref[:, :LANES] = jnp.sum(tiles(p_sum), axis=0, keepdims=True)
    psum_ref[:, LANES:] = jnp.sum(tiles(pa_sum), axis=0, keepdims=True)


def columns_kernel(
    rows_total, got_ref, rows_ref, g_ref, ga_ref, state_ref, attn_state_ref,
    cols_ref, attn_cols_ref, kept_ref, sent_ref, lane_ref,
):
    rows, cols = g_ref.shape
    attn_cols = ga_ref.shape[0]
    half = rows // 2
    core = lax.axis_index(CORE)
    total = added(got_ref)
    row_sums = rows_ref[...]
    cols_new = KEEP * state_ref[...].reshape(1, cols) + (1.0 - KEEP) * (total[:, :cols] / rows_total)
    cols_ref[...] = cols_new.reshape(cols)
    attn_state = attn_state_ref[...].reshape(1, attn_cols)
    attn_new = KEEP * attn_state + (1.0 - KEEP) * (total[:, cols : cols + attn_cols] / rows_total)
    attn_cols_ref[...] = attn_new.reshape(attn_cols)
    inverse = jnp.broadcast_to(1.0 / cols_new, (SLAB, cols))
    attn_inverse = jnp.concatenate([1.0 / attn_new, jnp.ones((1, 2 * LANES - attn_cols), F32)], axis=1)
    down_inverse = [down(attn_inverse[:, k * LANES : (k + 1) * LANES]) for k in range(2)]

    def step(s, carry):
        g = g_ref[pl.ds(s * SLAB, SLAB), :].astype(F32)
        lane_ref[pl.ds(s * SLAB, SLAB), :] = tiles(g * g * inverse)
        return carry

    lax.fori_loop(0, rows // SLAB, step, 0, unroll=8)
    w_attn = jnp.zeros((8, rows), F32)
    for s in range(attn_cols // SLAB):
        g = ga_ref[pl.ds(s * SLAB, SLAB), :].astype(F32)
        at = s * SLAB
        scale = down_inverse[at // LANES][at % LANES : at % LANES + SLAB]
        w_attn = w_attn + fold(g * g * wide(scale, rows))
    w_attn = jnp.sum(w_attn, axis=0, keepdims=True)
    w_mlp = jnp.concatenate([turned_sum(lane_ref, b * LANES) for b in range(rows // LANES)], axis=1)
    vectors = (row_sums[:, :rows], row_sums[:, rows:], w_mlp, w_attn)
    first = jnp.concatenate([v[:, :half] for v in vectors], axis=1)
    last = jnp.concatenate([v[:, half:] for v in vectors], axis=1)
    kept_ref[...] = jnp.where(core == 0, first, last)
    sent_ref[...] = jnp.where(core == 0, last, first)


def spread_kernel(kept_ref, got_ref, psum_ref, sent_ref):
    value = jnp.concatenate([kept_ref[...] + got_ref[...], psum_ref[...]], axis=1)
    for k in range(sent_ref.shape[0]):
        sent_ref[k] = value


def rows_kernel(widths, got_ref, state_ref, attn_state_ref, sent_ref):
    rows = state_ref.shape[0]
    half = rows // 2
    core = lax.axis_index(CORE)
    total = added(got_ref)
    new, parts = [], []
    for k, (ref, width) in enumerate(zip((state_ref, attn_state_ref), widths)):
        state = ref[...].reshape(1, rows)
        state = jnp.where(core == 0, state[:, :half], state[:, half:])
        new.append(KEEP * state + (1.0 - KEEP) * (total[:, k * half : (k + 1) * half] / width))
        parts.append(tiles(total[:, (2 + k) * half : (3 + k) * half] / new[k]))
    value = jnp.concatenate([*parts, total[:, 4 * half :], *new], axis=1)
    for k in range(sent_ref.shape[0]):
        sent_ref[k] = value


def factor(got_ref, matrix, count):
    total = got_ref[0, :, : 4 * LANES]
    for k in range(1, got_ref.shape[0]):
        total = total + got_ref[k, :, : 4 * LANES]
    q, p = (
        jnp.broadcast_to(jnp.sum(total[:, k * LANES : (k + 1) * LANES], axis=1, keepdims=True), (1, LANES))
        for k in (matrix, 2 + matrix)
    )
    return LEARN_RATE * jnp.sqrt(p / count) / jnp.maximum(1.0, jnp.sqrt(q / count))


def new_rows(got_ref, matrix, half):
    row = lax.axis_index("row_0") * lax.axis_size("row_1") + lax.axis_index("row_1")
    at = pl.ds(4 * LANES + matrix * half, half)
    return jnp.concatenate([got_ref[2 * row, :, at], got_ref[2 * row + 1, :, at]], axis=1)


def attn_kernel(count, got_ref, attn_cols_ref, ga_ref, pa_ref, attn_ref, block_ref):
    attn_cols, rows = ga_ref.shape
    along = jnp.broadcast_to(lax.rsqrt(new_rows(got_ref, 1, rows // 2)), (SLAB, rows))
    across = attn_cols_ref[...].reshape(1, attn_cols)
    across = lax.rsqrt(jnp.concatenate([across, jnp.ones((1, 2 * LANES - attn_cols), F32)], axis=1))
    scale = factor(got_ref, 1, count)
    across = [down(across[:, k * LANES : (k + 1) * LANES] * scale) for k in range(2)]
    for s in range(attn_cols // SLAB):
        at = s * SLAB
        scale = across[at // LANES][at % LANES : at % LANES + SLAB]
        new = pa_ref[pl.ds(at, SLAB), :] - ga_ref[pl.ds(at, SLAB), :].astype(F32) * wide(scale, rows) * along
        attn_ref[pl.ds(at, SLAB), :] = new
        block_ref[pl.ds(at, SLAB), :] = new.astype(BF16)


def place(dx, dy):
    x = lax.rem(lax.axis_index("row_0") + dx, lax.axis_size("row_0"))
    y = lax.rem(lax.axis_index("row_1") + dy, lax.axis_size("row_1"))
    return x * lax.axis_size("row_1") + y


def fill_kernel(offsets, *refs):
    blocks, out_hbm, sems = refs[: len(offsets)], refs[-2], refs[-1]
    width = blocks[0].shape[1]
    copies = []
    for k, (ref, offset) in enumerate(zip(blocks, offsets)):
        at = pl.multiple_of(place(*offset) * width, width)
        copies.append(pltpu.make_async_copy(ref, out_hbm.at[:, pl.ds(at, width)], sems.at[k]))
        copies[-1].start()
    for copy in copies:
        copy.wait()


def fill(copy, offsets, blocks):
    count = len(blocks)
    return call(
        functools.partial(fill_kernel, offsets),
        [jax.ShapeDtypeStruct(copy.shape, copy.dtype)],
        (*blocks, copy),
        in_specs=[ON_CHIP] * count + [OFF_CHIP],
        out_specs=[OFF_CHIP],
        scratch=[pltpu.SemaphoreType.DMA((count,))],
        aliases={count: 0},
    )[0]


def finish_kernel(
    count, block_ref, got_ref, cols_ref, attn_cols_ref, attn_ref, g_ref, p_ref,
    copy_hbm, attn_hbm, new_hbm, rows_hbm, cols_hbm, attn_rows_hbm, attn_cols_hbm,
    new_ref, rows_ref, attn_rows_ref, sems,
):
    rows, cols = g_ref.shape
    blocks = rows // LANES
    copies = []

    def put(source, target):
        copies.append(pltpu.make_async_copy(source, target, sems.at[len(copies)]))
        copies[-1].start()

    put(block_ref, copy_hbm.at[:, pl.ds(pl.multiple_of(place(0, 0) * rows, rows), rows)])
    put(attn_ref, attn_hbm)
    put(cols_ref, cols_hbm)
    put(attn_cols_ref, attn_cols_hbm)
    row_factors = new_rows(got_ref, 0, rows // 2)
    rows_ref[...] = row_factors.reshape(rows)
    attn_rows_ref[...] = new_rows(got_ref, 1, rows // 2).reshape(rows)
    along = jnp.broadcast_to(lax.rsqrt(cols_ref[...].reshape(1, cols)), (SLAB, cols))
    scale = factor(got_ref, 0, count)
    row_scale = lax.rsqrt(row_factors)
    for b in range(blocks):
        across = down(row_scale[:, b * LANES : (b + 1) * LANES] * scale)
        for s in range(LANES // SLAB):
            at = pl.ds(b * LANES + s * SLAB, SLAB)
            new_ref[at, :] = (
                p_ref[at, :] - g_ref[at, :].astype(F32) * wide(across[s * SLAB : (s + 1) * SLAB], cols) * along
            )
        at = pl.ds(b * LANES, LANES)
        put(new_ref.at[at], new_hbm.at[at])
    put(rows_ref, rows_hbm)
    put(attn_rows_ref, attn_rows_hbm)
    for copy in copies:
        copy.wait()


def everyone(value, axes):
    return lax.all_to_all(value, axes, 0, 0, tiled=True)


def moved(value, dx, dy):
    xs, ys = lax.axis_size("row_0"), lax.axis_size("row_1")
    pairs = [(x * ys + y, (x + dx) % xs * ys + (y + dy) % ys) for x in range(xs) for y in range(ys)]
    return lax.ppermute(value, ROW, pairs)


def other_core(value):
    return lax.ppermute(value, CORE, [(0, 1), (1, 0)])


def local(
    mlp_param,
    mlp_grad,
    mlp_row_state,
    mlp_col_state,
    attn_param,
    attn_grad,
    attn_row_state,
    attn_col_state,
):
    rows, cols = mlp_grad.shape
    attn_cols = attn_grad.shape[1]
    half = rows // 2
    row_devices, layers = lax.axis_size(ROW), lax.axis_size(LAYERS)
    message = -(-(cols + attn_cols) // LANES) * LANES
    rows_total = rows * row_devices
    widths = (float(cols * lax.axis_size(COL)), float(attn_cols * lax.axis_size(COL)))
    counts = (rows_total * widths[0], rows_total * widths[1])
    attn_grad, attn_param = attn_grad.T, attn_param.T
    blocks = rows // LANES

    sent, row_sums, p_sums, g, ga, p, pa = call(
        sums_kernel,
        [
            pltpu.VMEM((row_devices, 1, message), F32),
            pltpu.VMEM((1, 2 * rows), F32),
            pltpu.VMEM((1, 2 * LANES), F32),
            pltpu.VMEM((rows, cols), BF16),
            pltpu.VMEM((attn_cols, rows), BF16),
            pltpu.VMEM((rows, cols), F32),
            pltpu.VMEM((attn_cols, rows), F32),
        ],
        (mlp_grad, attn_grad, mlp_param, attn_param),
        in_specs=[OFF_CHIP] * 4,
        scratch=[
            pltpu.VMEM((rows + 2 * LANES, LANES), F32),
            pltpu.SemaphoreType.DMA((2 * blocks + 2,)),
        ],
        limit=119 << 19,
    )
    got = everyone(sent, ROW)
    cols_new, attn_cols_new, kept, sent = call(
        functools.partial(columns_kernel, float(rows_total)),
        [
            pltpu.VMEM((cols,), F32),
            pltpu.VMEM((attn_cols,), F32),
            pltpu.VMEM((1, 4 * half), F32),
            pltpu.VMEM((1, 4 * half), F32),
        ],
        (got, row_sums, g, ga, mlp_col_state, attn_col_state),
        scratch=[pltpu.VMEM((rows, LANES), F32)],
    )
    (sent,) = call(
        spread_kernel,
        [pltpu.VMEM((layers, 1, 4 * half + 2 * LANES), F32)],
        (kept, other_core(sent), p_sums),
    )
    (sent,) = call(
        functools.partial(rows_kernel, widths),
        [pltpu.VMEM((2 * row_devices, 1, 4 * LANES + 2 * half), F32)],
        (everyone(sent, LAYERS), mlp_row_state, attn_row_state),
    )
    got = everyone(sent, (*ROW, CORE))
    attn_new, block = call(
        functools.partial(attn_kernel, counts[1]),
        [pltpu.VMEM((attn_cols, rows), F32), pltpu.VMEM((attn_cols, rows), BF16)],
        (got, attn_cols_new, ga, pa),
    )
    across = moved(block, 2, 0)
    partner = moved(block, 0, 1)
    left, right = moved(block, 1, 0), moved(block, 3, 0)
    partner_across = moved(across, 0, 1)
    partner_left, partner_right = moved(partner, 1, 0), moved(partner, 3, 0)
    copy, attn_new, mlp_new, rows_new, cols_new, attn_rows_new, attn_cols_new = call(
        functools.partial(finish_kernel, counts[0]),
        [
            jax.ShapeDtypeStruct((attn_cols, rows_total), BF16),
            jax.ShapeDtypeStruct((attn_cols, rows), F32),
            jax.ShapeDtypeStruct((rows, cols), F32),
            jax.ShapeDtypeStruct((rows,), F32),
            jax.ShapeDtypeStruct((cols,), F32),
            jax.ShapeDtypeStruct((rows,), F32),
            jax.ShapeDtypeStruct((attn_cols,), F32),
        ],
        (block, got, cols_new, attn_cols_new, attn_new, g, p),
        out_specs=[OFF_CHIP] * 7,
        scratch=[
            pltpu.VMEM((rows, cols), F32),
            pltpu.VMEM((rows,), F32),
            pltpu.VMEM((rows,), F32),
            pltpu.SemaphoreType.DMA((blocks + 6,)),
        ],
        flops=1 << 22,
    )
    copy = fill(copy, ((2, 0), (0, 1), (3, 0), (1, 0)), (across, partner, left, right))
    copy = fill(copy, ((2, 1), (3, 1), (1, 1)), (partner_across, partner_left, partner_right))
    return mlp_new, attn_new.T, rows_new, cols_new, attn_rows_new, attn_cols_new, copy.T


def solution(mesh):
    finer = Mesh(mesh.devices.reshape(4, 2, 2, 8, 2), (*ROW, *COL))
    return jax.shard_map(
        local,
        mesh=finer,
        in_specs=(
            P(ROW, COL),
            P(ROW, COL),
            P(ROW),
            P(COL),
            P(ROW, COL),
            P(ROW, COL),
            P(ROW),
            P(COL),
        ),
        out_specs=(P(ROW, COL), P(ROW, COL), P(ROW), P(COL), P(ROW), P(COL), P(None, COL)),
        check_vma=False,
    )
```

```python
import functools

import jax
import jax.numpy as jnp
from jax import lax
from jax.experimental import pallas as pl
from jax.experimental.pallas import tpu as pltpu
from jax.sharding import Mesh
from jax.sharding import PartitionSpec as P

STEP = 4
ROW = ("row_0", "row_1")
COL = ("col_0", "col_1", "col_2")
Y_HI, Z, CORE = COL
LAYERS = (Y_HI, Z)

TINY_SQUARE = 1e-30
LEARN_RATE = 0.05
DECAY_POWER = 0.8
KEEP = 1.0 - STEP ** (-DECAY_POWER)

F32, BF16 = jnp.float32, jnp.bfloat16
SLAB = 16
LANES = 128
ON_CHIP = pl.BlockSpec(memory_space=pltpu.VMEM)
OFF_CHIP = pl.BlockSpec(memory_space=pltpu.HBM)


def call(kernel, outs, args, in_specs=None, out_specs=None, scratch=(), limit=4 << 20, aliases=None, flops=0):
    return pl.pallas_call(
        kernel,
        out_shape=outs,
        in_specs=in_specs or [ON_CHIP] * len(args),
        out_specs=out_specs or [ON_CHIP] * len(outs),
        scratch_shapes=scratch,
        input_output_aliases=aliases or {},
        cost_estimate=pl.CostEstimate(flops=flops, bytes_accessed=flops, transcendentals=0) if flops else None,
        compiler_params=pltpu.CompilerParams(vmem_limit_bytes=limit),
    )(*args)


def tiles(value):
    width = value.shape[1] // LANES
    return sum((value[:, k * LANES : (k + 1) * LANES] for k in range(1, width)), value[:, :LANES])


def wide(value, width):
    return jnp.concatenate([value] * (width // LANES), axis=1)


def turned_sum(ref, start):
    return jnp.sum(ref[pl.ds(start, LANES), :].T, axis=0, keepdims=True)


def down(value):
    return jnp.broadcast_to(value, (LANES, LANES)).T


def fold(value):
    return value[:8] + value[8:]


def added(ref):
    total = ref[0]
    for k in range(1, ref.shape[0]):
        total = total + ref[k]
    return total


def sums_kernel(
    g_hbm, ga_hbm, p_hbm, pa_hbm, sent_ref, rows_ref, psum_ref, g_ref, ga_ref, p_ref, pa_ref, lane_ref, sems
):
    rows, cols = g_hbm.shape
    attn_cols = ga_hbm.shape[0]
    blocks = rows // LANES
    g_copies = [
        pltpu.make_async_copy(g_hbm.at[pl.ds(b * LANES, LANES)], g_ref.at[pl.ds(b * LANES, LANES)], sems.at[b])
        for b in range(blocks)
    ]
    p_copies = [
        pltpu.make_async_copy(
            p_hbm.at[pl.ds(b * LANES, LANES)], p_ref.at[pl.ds(b * LANES, LANES)], sems.at[blocks + b]
        )
        for b in range(blocks)
    ]
    ga_copy = pltpu.make_async_copy(ga_hbm, ga_ref, sems.at[2 * blocks])
    pa_copy = pltpu.make_async_copy(pa_hbm, pa_ref, sems.at[2 * blocks + 1])
    for copy in (*g_copies, ga_copy, *p_copies, pa_copy):
        copy.start()
    lane_ref[pl.ds(rows, 2 * LANES), :] = jnp.zeros((2 * LANES, LANES), F32)

    def squares(ref, start, first):
        def step(s, acc):
            g = ref[pl.ds(start + s * SLAB, SLAB), :].astype(F32)
            g = g * g
            lane_ref[pl.ds(first + start + s * SLAB, SLAB), :] = tiles(g)
            return acc + fold(g)

        return step

    def own_squares(ref, start):
        def step(s, acc):
            p = ref[pl.ds(start + s * SLAB, SLAB), :]
            return acc + fold(p * p)

        return step

    eight = jnp.zeros((8, cols), F32)
    steps = LANES // SLAB
    col_sum = eight
    for b, copy in enumerate(g_copies):
        copy.wait()
        col_sum = lax.fori_loop(0, steps, squares(g_ref, b * LANES, 0), col_sum, unroll=True)
        rows_ref[:, pl.ds(b * LANES, LANES)] = turned_sum(lane_ref, b * LANES)
    ga_copy.wait()
    row_sum = lax.fori_loop(0, attn_cols // SLAB, squares(ga_ref, 0, rows), jnp.zeros((8, rows), F32), unroll=4)
    rows_ref[:, pl.ds(rows, rows)] = jnp.sum(row_sum, axis=0, keepdims=True)
    rows_ref[...] += jnp.concatenate(
        [jnp.full((1, rows), cols * TINY_SQUARE, F32), jnp.full((1, rows), attn_cols * TINY_SQUARE, F32)], axis=1
    )
    col_sums = jnp.concatenate(
        [
            jnp.sum(col_sum, axis=0, keepdims=True),
            turned_sum(lane_ref, rows),
            turned_sum(lane_ref, rows + LANES),
        ],
        axis=1,
    ) + rows * TINY_SQUARE
    for k in range(sent_ref.shape[0]):
        sent_ref[k] = col_sums
    p_sum = eight
    for b, copy in enumerate(p_copies):
        copy.wait()
        p_sum = lax.fori_loop(0, steps, own_squares(p_ref, b * LANES), p_sum, unroll=True)
    pa_copy.wait()
    pa_sum = lax.fori_loop(0, attn_cols // SLAB, own_squares(pa_ref, 0), jnp.zeros((8, rows), F32), unroll=4)
    psum_ref[:, :LANES] = jnp.sum(tiles(p_sum), axis=0, keepdims=True)
    psum_ref[:, LANES:] = jnp.sum(tiles(pa_sum), axis=0, keepdims=True)


def columns_kernel(
    rows_total, got_ref, rows_ref, g_ref, ga_ref, pa_ref, state_ref, attn_state_ref,
    cols_ref, attn_cols_ref, kept_ref, sent_ref, early_ref, lane_ref,
):
    rows, cols = g_ref.shape
    attn_cols = ga_ref.shape[0]
    half = rows // 2
    core = lax.axis_index(CORE)
    total = added(got_ref)
    row_sums = rows_ref[...]
    cols_new = KEEP * state_ref[...].reshape(1, cols) + (1.0 - KEEP) * (total[:, :cols] / rows_total)
    cols_ref[...] = cols_new.reshape(cols)
    attn_state = attn_state_ref[...].reshape(1, attn_cols)
    attn_new = KEEP * attn_state + (1.0 - KEEP) * (total[:, cols : cols + attn_cols] / rows_total)
    attn_cols_ref[...] = attn_new.reshape(attn_cols)
    inverse = jnp.broadcast_to(1.0 / cols_new, (SLAB, cols))
    attn_inverse = jnp.concatenate([1.0 / attn_new, jnp.ones((1, 2 * LANES - attn_cols), F32)], axis=1)
    down_inverse = [down(attn_inverse[:, k * LANES : (k + 1) * LANES]) for k in range(2)]

    def step(s, carry):
        g = g_ref[pl.ds(s * SLAB, SLAB), :].astype(F32)
        lane_ref[pl.ds(s * SLAB, SLAB), :] = tiles(g * g * inverse)
        return carry

    lax.fori_loop(0, rows // SLAB, step, 0, unroll=8)
    w_attn = jnp.zeros((8, rows), F32)
    for s in range(attn_cols // SLAB):
        g = ga_ref[pl.ds(s * SLAB, SLAB), :].astype(F32)
        at = s * SLAB
        scale = down_inverse[at // LANES][at % LANES : at % LANES + SLAB]
        w_attn = w_attn + fold(g * g * wide(scale, rows))
    w_attn = jnp.sum(w_attn, axis=0, keepdims=True)
    w_mlp = jnp.concatenate([turned_sum(lane_ref, b * LANES) for b in range(rows // LANES)], axis=1)
    vectors = (row_sums[:, :rows], row_sums[:, rows:], w_mlp, w_attn)
    first = jnp.concatenate([v[:, :half] for v in vectors], axis=1)
    last = jnp.concatenate([v[:, half:] for v in vectors], axis=1)
    early = early_ref.shape[0] // 3
    for at in range(0, early, SLAB):
        p = pa_ref[pl.ds(at, SLAB), :]
        high = p.astype(BF16)
        early_ref[pl.ds(at, SLAB), :] = high
        early_ref[pl.ds(early + at, SLAB), :] = (p - high.astype(F32)).astype(BF16)
    early_ref[pl.ds(2 * early, early), :] = ga_ref[pl.ds(0, early), :]
    kept_ref[...] = jnp.where(core == 0, first, last)
    sent_ref[...] = jnp.where(core == 0, last, first)


def spread_kernel(kept_ref, got_ref, psum_ref, sent_ref):
    value = jnp.concatenate([kept_ref[...] + got_ref[...], psum_ref[...]], axis=1)
    for k in range(sent_ref.shape[0]):
        sent_ref[k] = value


def rows_kernel(widths, got_ref, state_ref, attn_state_ref, sent_ref):
    rows = state_ref.shape[0]
    half = rows // 2
    core = lax.axis_index(CORE)
    total = added(got_ref)
    new, parts = [], []
    for k, (ref, width) in enumerate(zip((state_ref, attn_state_ref), widths)):
        state = ref[...].reshape(1, rows)
        state = jnp.where(core == 0, state[:, :half], state[:, half:])
        new.append(KEEP * state + (1.0 - KEEP) * (total[:, k * half : (k + 1) * half] / width))
        parts.append(tiles(total[:, (2 + k) * half : (3 + k) * half] / new[k]))
    value = jnp.concatenate([*parts, total[:, 4 * half :], *new], axis=1)
    for k in range(sent_ref.shape[0]):
        sent_ref[k] = value


def factor(got_ref, matrix, count):
    total = got_ref[0, :, : 4 * LANES]
    for k in range(1, got_ref.shape[0]):
        total = total + got_ref[k, :, : 4 * LANES]
    q, p = (
        jnp.broadcast_to(jnp.sum(total[:, k * LANES : (k + 1) * LANES], axis=1, keepdims=True), (1, LANES))
        for k in (matrix, 2 + matrix)
    )
    return LEARN_RATE * jnp.sqrt(p / count) / jnp.maximum(1.0, jnp.sqrt(q / count))


def new_rows(got_ref, matrix, half, dx=0):
    row = place(dx, 0)
    at = pl.ds(4 * LANES + matrix * half, half)
    return jnp.concatenate([got_ref[2 * row, :, at], got_ref[2 * row + 1, :, at]], axis=1)


def attn_scales(count, got_ref, attn_cols_ref):
    attn_cols = attn_cols_ref.shape[0]
    across = attn_cols_ref[...].reshape(1, attn_cols)
    across = lax.rsqrt(jnp.concatenate([across, jnp.ones((1, 2 * LANES - attn_cols), F32)], axis=1))
    scale = factor(got_ref, 1, count)
    return [down(across[:, k * LANES : (k + 1) * LANES] * scale) for k in range(2)]


def attn_new(g, p, at, across, along):
    scale = across[at // LANES][at % LANES : at % LANES + SLAB]
    return p - g * wide(scale, g.shape[1]) * along


def attn_kernel(count, got_ref, attn_cols_ref, ga_ref, pa_ref, attn_ref, block_ref, rest_ref):
    attn_cols, rows = ga_ref.shape
    early = attn_cols - rest_ref.shape[0]
    across = attn_scales(count, got_ref, attn_cols_ref)
    along = jnp.broadcast_to(lax.rsqrt(new_rows(got_ref, 1, rows // 2)), (SLAB, rows))
    for at in range(0, attn_cols, SLAB):
        rows_at = pl.ds(at, SLAB)
        value = attn_new(ga_ref[rows_at, :].astype(F32), pa_ref[rows_at, :], at, across, along)
        attn_ref[pl.ds(at, SLAB), :] = value
        block_ref[pl.ds(at, SLAB), :] = value.astype(BF16)
        if at >= early:
            rest_ref[pl.ds(at - early, SLAB), :] = value.astype(BF16)


def early_kernel(count, got_ref, attn_cols_ref, ahead_ref, out_ref):
    early, rows = out_ref.shape
    across = attn_scales(count, got_ref, attn_cols_ref)
    along = jnp.broadcast_to(lax.rsqrt(new_rows(got_ref, 1, rows // 2, 2)), (SLAB, rows))
    for at in range(0, early, SLAB):
        high, low, g = (ahead_ref[pl.ds(k * early + at, SLAB), :].astype(F32) for k in range(3))
        out_ref[pl.ds(at, SLAB), :] = attn_new(g, high + low, at, across, along).astype(BF16)


def place(dx, dy):
    x = lax.rem(lax.axis_index("row_0") + dx, lax.axis_size("row_0"))
    y = lax.rem(lax.axis_index("row_1") + dy, lax.axis_size("row_1"))
    return x * lax.axis_size("row_1") + y


def fill_kernel(offsets, *refs):
    blocks, out_hbm, sems = refs[: len(offsets)], refs[-2], refs[-1]
    width = blocks[0].shape[1]
    copies = []
    for k, (ref, offset) in enumerate(zip(blocks, offsets)):
        dx, dy, first = offset
        at = pl.multiple_of(place(dx, dy) * width, width)
        target = out_hbm.at[pl.ds(first, ref.shape[0]), pl.ds(at, width)]
        copies.append(pltpu.make_async_copy(ref, target, sems.at[k]))
        copies[-1].start()
    for copy in copies:
        copy.wait()


def fill(copy, offsets, blocks):
    count = len(blocks)
    return call(
        functools.partial(fill_kernel, offsets),
        [jax.ShapeDtypeStruct(copy.shape, copy.dtype)],
        (*blocks, copy),
        in_specs=[ON_CHIP] * count + [OFF_CHIP],
        out_specs=[OFF_CHIP],
        scratch=[pltpu.SemaphoreType.DMA((count,))],
        aliases={count: 0},
    )[0]


def finish_kernel(
    count, block_ref, got_ref, cols_ref, attn_cols_ref, attn_ref, g_ref, p_ref,
    copy_hbm, attn_hbm, new_hbm, rows_hbm, cols_hbm, attn_rows_hbm, attn_cols_hbm,
    new_ref, rows_ref, attn_rows_ref, sems,
):
    rows, cols = g_ref.shape
    blocks = rows // LANES
    copies = []

    def put(source, target):
        copies.append(pltpu.make_async_copy(source, target, sems.at[len(copies)]))
        copies[-1].start()

    put(block_ref, copy_hbm.at[:, pl.ds(pl.multiple_of(place(0, 0) * rows, rows), rows)])
    put(attn_ref, attn_hbm)
    put(cols_ref, cols_hbm)
    put(attn_cols_ref, attn_cols_hbm)
    row_factors = new_rows(got_ref, 0, rows // 2)
    rows_ref[...] = row_factors.reshape(rows)
    attn_rows_ref[...] = new_rows(got_ref, 1, rows // 2).reshape(rows)
    along = jnp.broadcast_to(lax.rsqrt(cols_ref[...].reshape(1, cols)), (SLAB, cols))
    scale = factor(got_ref, 0, count)
    row_scale = lax.rsqrt(row_factors)
    for b in range(blocks):
        across = down(row_scale[:, b * LANES : (b + 1) * LANES] * scale)
        for s in range(LANES // SLAB):
            at = pl.ds(b * LANES + s * SLAB, SLAB)
            new_ref[at, :] = (
                p_ref[at, :] - g_ref[at, :].astype(F32) * wide(across[s * SLAB : (s + 1) * SLAB], cols) * along
            )
        at = pl.ds(b * LANES, LANES)
        put(new_ref.at[at], new_hbm.at[at])
    put(rows_ref, rows_hbm)
    put(attn_rows_ref, attn_rows_hbm)
    for copy in copies:
        copy.wait()


def everyone(value, axes):
    return lax.all_to_all(value, axes, 0, 0, tiled=True)


def moved(value, dx, dy):
    xs, ys = lax.axis_size("row_0"), lax.axis_size("row_1")
    pairs = [(x * ys + y, (x + dx) % xs * ys + (y + dy) % ys) for x in range(xs) for y in range(ys)]
    return lax.ppermute(value, ROW, pairs)


def other_core(value):
    return lax.ppermute(value, CORE, [(0, 1), (1, 0)])


def step(
    mlp_param,
    mlp_grad,
    mlp_row_state,
    mlp_col_state,
    attn_param,
    attn_grad,
    attn_row_state,
    attn_col_state,
):
    rows, cols = mlp_grad.shape
    attn_cols = attn_grad.shape[1]
    half = rows // 2
    row_devices, layers = lax.axis_size(ROW), lax.axis_size(LAYERS)
    message = -(-(cols + attn_cols) // LANES) * LANES
    rows_total = rows * row_devices
    widths = (float(cols * lax.axis_size(COL)), float(attn_cols * lax.axis_size(COL)))
    counts = (rows_total * widths[0], rows_total * widths[1])
    attn_grad, attn_param = attn_grad.T, attn_param.T
    blocks = rows // LANES
    early = attn_cols // 2 // SLAB * SLAB

    sent, row_sums, p_sums, g, ga, p, pa = call(
        sums_kernel,
        [
            pltpu.VMEM((row_devices, 1, message), F32),
            pltpu.VMEM((1, 2 * rows), F32),
            pltpu.VMEM((1, 2 * LANES), F32),
            pltpu.VMEM((rows, cols), BF16),
            pltpu.VMEM((attn_cols, rows), BF16),
            pltpu.VMEM((rows, cols), F32),
            pltpu.VMEM((attn_cols, rows), F32),
        ],
        (mlp_grad, attn_grad, mlp_param, attn_param),
        in_specs=[OFF_CHIP] * 4,
        scratch=[
            pltpu.VMEM((rows + 2 * LANES, LANES), F32),
            pltpu.SemaphoreType.DMA((2 * blocks + 2,)),
        ],
        limit=119 << 19,
    )
    got = everyone(sent, ROW)
    cols_new, attn_cols_new, kept, sent, ahead = call(
        functools.partial(columns_kernel, float(rows_total)),
        [
            pltpu.VMEM((cols,), F32),
            pltpu.VMEM((attn_cols,), F32),
            pltpu.VMEM((1, 4 * half), F32),
            pltpu.VMEM((1, 4 * half), F32),
            pltpu.VMEM((3 * early, rows), BF16),
        ],
        (got, row_sums, g, ga, pa, mlp_col_state, attn_col_state),
        scratch=[pltpu.VMEM((rows, LANES), F32)],
    )
    swapped = other_core(sent)
    (sent,) = call(
        spread_kernel,
        [pltpu.VMEM((layers, 1, 4 * half + 2 * LANES), F32)],
        (kept, swapped, p_sums),
    )
    got = everyone(sent, LAYERS)
    (sent,) = call(
        functools.partial(rows_kernel, widths),
        [pltpu.VMEM((2 * row_devices, 1, 4 * LANES + 2 * half), F32)],
        (got, mlp_row_state, attn_row_state),
    )
    got = everyone(sent, (*ROW, CORE))
    ahead = moved(ahead, 2, 0)
    attn_new, block, rest = call(
        functools.partial(attn_kernel, counts[1]),
        [
            pltpu.VMEM((attn_cols, rows), F32),
            pltpu.VMEM((attn_cols, rows), BF16),
            pltpu.VMEM((attn_cols - early, rows), BF16),
        ],
        (got, attn_cols_new, ga, pa),
    )
    (first_across,) = call(
        functools.partial(early_kernel, counts[1]),
        [pltpu.VMEM((early, rows), BF16)],
        (got, attn_cols_new, ahead),
    )
    across = moved(rest, 2, 0)
    partner = moved(block, 0, 1)
    left, right = moved(block, 1, 0), moved(block, 3, 0)
    partner_first = moved(first_across, 0, 1)
    partner_across = moved(across, 0, 1)
    partner_left = moved(partner, 1, 0)
    partner_right = moved(partner, 3, 0)
    copy, attn_new, mlp_new, rows_new, cols_new, attn_rows_new, attn_cols_new = call(
        functools.partial(finish_kernel, counts[0]),
        [
            jax.ShapeDtypeStruct((attn_cols, rows_total), BF16),
            jax.ShapeDtypeStruct((attn_cols, rows), F32),
            jax.ShapeDtypeStruct((rows, cols), F32),
            jax.ShapeDtypeStruct((rows,), F32),
            jax.ShapeDtypeStruct((cols,), F32),
            jax.ShapeDtypeStruct((rows,), F32),
            jax.ShapeDtypeStruct((attn_cols,), F32),
        ],
        (block, got, cols_new, attn_cols_new, attn_new, g, p),
        out_specs=[OFF_CHIP] * 7,
        scratch=[
            pltpu.VMEM((rows, cols), F32),
            pltpu.VMEM((rows,), F32),
            pltpu.VMEM((rows,), F32),
            pltpu.SemaphoreType.DMA((blocks + 6,)),
        ],
        flops=1 << 22,
    )
    copy = fill(
        copy,
        ((2, 0, 0), (2, 0, early), (0, 1, 0), (3, 0, 0), (1, 0, 0)),
        (first_across, across, partner, left, right),
    )
    copy = fill(
        copy,
        ((2, 1, 0), (2, 1, early), (3, 1, 0), (1, 1, 0)),
        (partner_first, partner_across, partner_left, partner_right),
    )
    return mlp_new, attn_new.T, rows_new, cols_new, attn_rows_new, attn_cols_new, copy.T


def solution(mesh):
    finer = Mesh(mesh.devices.reshape(4, 2, 2, 8, 2), (*ROW, *COL))
    return jax.shard_map(
        step,
        mesh=finer,
        in_specs=(
            P(ROW, COL),
            P(ROW, COL),
            P(ROW),
            P(COL),
            P(ROW, COL),
            P(ROW, COL),
            P(ROW),
            P(COL),
        ),
        out_specs=(P(ROW, COL), P(ROW, COL), P(ROW), P(COL), P(ROW), P(COL), P(None, COL)),
        check_vma=False,
    )
```

```python
import functools

import jax
import jax.numpy as jnp
from jax import lax
from jax.experimental import pallas as pl
from jax.experimental.pallas import tpu as pltpu
from jax.sharding import Mesh
from jax.sharding import PartitionSpec as P

STEP = 4
ROW = ("row_0", "row_1")
COL = ("col_0", "col_1", "col_2")
Y_HI, Z, CORE = COL
LAYERS = (Y_HI, Z)

TINY_SQUARE = 1e-30
LEARN_RATE = 0.05
DECAY_POWER = 0.8
KEEP = 1.0 - STEP ** (-DECAY_POWER)

F32, BF16 = jnp.float32, jnp.bfloat16
SLAB = 16
LANES = 128
ON_CHIP = pl.BlockSpec(memory_space=pltpu.VMEM)
OFF_CHIP = pl.BlockSpec(memory_space=pltpu.HBM)


def call(kernel, outs, args, in_specs=None, out_specs=None, scratch=(), limit=4 << 20, aliases=None, flops=0):
    return pl.pallas_call(
        kernel,
        out_shape=outs,
        in_specs=in_specs or [ON_CHIP] * len(args),
        out_specs=out_specs or [ON_CHIP] * len(outs),
        scratch_shapes=scratch,
        input_output_aliases=aliases or {},
        cost_estimate=pl.CostEstimate(flops=flops, bytes_accessed=flops, transcendentals=0) if flops else None,
        compiler_params=pltpu.CompilerParams(vmem_limit_bytes=limit),
    )(*args)


def tiles(value):
    width = value.shape[1] // LANES
    return sum((value[:, k * LANES : (k + 1) * LANES] for k in range(1, width)), value[:, :LANES])


def wide(value, width):
    return jnp.concatenate([value] * (width // LANES), axis=1)


def turned_sum(ref, start):
    return jnp.sum(ref[pl.ds(start, LANES), :].T, axis=0, keepdims=True)


def down(value):
    return jnp.broadcast_to(value, (LANES, LANES)).T


def fold(value):
    return value[:8] + value[8:]


def added(ref):
    total = ref[0]
    for k in range(1, ref.shape[0]):
        total = total + ref[k]
    return total


def sums_kernel(
    g_hbm, ga_hbm, p_hbm, pa_hbm, sent_ref, rows_ref, psum_ref, g_ref, ga_ref, p_ref, pa_ref, lane_ref, sems
):
    rows, cols = g_hbm.shape
    attn_cols = ga_hbm.shape[0]
    blocks = rows // LANES
    g_copies = [
        pltpu.make_async_copy(g_hbm.at[pl.ds(b * LANES, LANES)], g_ref.at[pl.ds(b * LANES, LANES)], sems.at[b])
        for b in range(blocks)
    ]
    p_copies = [
        pltpu.make_async_copy(
            p_hbm.at[pl.ds(b * LANES, LANES)], p_ref.at[pl.ds(b * LANES, LANES)], sems.at[blocks + b]
        )
        for b in range(blocks)
    ]
    ga_copy = pltpu.make_async_copy(ga_hbm, ga_ref, sems.at[2 * blocks])
    pa_copy = pltpu.make_async_copy(pa_hbm, pa_ref, sems.at[2 * blocks + 1])
    for copy in (ga_copy, *g_copies, *p_copies, pa_copy):
        copy.start()
    lane_ref[pl.ds(rows, 2 * LANES), :] = jnp.zeros((2 * LANES, LANES), F32)

    def squares(ref, start, first):
        def step(s, acc):
            g = ref[pl.ds(start + s * SLAB, SLAB), :].astype(F32)
            g = g * g
            lane_ref[pl.ds(first + start + s * SLAB, SLAB), :] = tiles(g)
            return acc + fold(g)

        return step

    def own_squares(ref, start):
        def step(s, acc):
            p = ref[pl.ds(start + s * SLAB, SLAB), :]
            return acc + fold(p * p)

        return step

    eight = jnp.zeros((8, cols), F32)
    ga_copy.wait()
    row_sum = lax.fori_loop(0, attn_cols // SLAB, squares(ga_ref, 0, rows), jnp.zeros((8, rows), F32), unroll=4)
    rows_ref[:, pl.ds(rows, rows)] = jnp.sum(row_sum, axis=0, keepdims=True)
    steps = LANES // SLAB
    col_sum = eight
    for b, copy in enumerate(g_copies):
        copy.wait()
        col_sum = lax.fori_loop(0, steps, squares(g_ref, b * LANES, 0), col_sum, unroll=True)
        rows_ref[:, pl.ds(b * LANES, LANES)] = turned_sum(lane_ref, b * LANES)
    rows_ref[...] += jnp.concatenate(
        [jnp.full((1, rows), cols * TINY_SQUARE, F32), jnp.full((1, rows), attn_cols * TINY_SQUARE, F32)], axis=1
    )
    col_sums = jnp.concatenate(
        [
            jnp.sum(col_sum, axis=0, keepdims=True),
            turned_sum(lane_ref, rows),
            turned_sum(lane_ref, rows + LANES),
        ],
        axis=1,
    ) + rows * TINY_SQUARE
    for k in range(sent_ref.shape[0]):
        sent_ref[k] = col_sums
    p_sum = eight
    for b, copy in enumerate(p_copies):
        copy.wait()
        p_sum = lax.fori_loop(0, steps, own_squares(p_ref, b * LANES), p_sum, unroll=True)
    pa_copy.wait()
    pa_sum = lax.fori_loop(0, attn_cols // SLAB, own_squares(pa_ref, 0), jnp.zeros((8, rows), F32), unroll=4)
    psum_ref[:, :LANES] = jnp.sum(tiles(p_sum), axis=0, keepdims=True)
    psum_ref[:, LANES:] = jnp.sum(tiles(pa_sum), axis=0, keepdims=True)


def columns_kernel(
    rows_total, got_ref, rows_ref, g_ref, ga_ref, pa_ref, state_ref, attn_state_ref,
    cols_ref, attn_cols_ref, kept_ref, sent_ref, early_ref, lane_ref,
):
    rows, cols = g_ref.shape
    attn_cols = ga_ref.shape[0]
    half = rows // 2
    core = lax.axis_index(CORE)
    total = added(got_ref)
    row_sums = rows_ref[...]
    cols_new = KEEP * state_ref[...].reshape(1, cols) + (1.0 - KEEP) * (total[:, :cols] / rows_total)
    cols_ref[...] = cols_new.reshape(cols)
    attn_state = attn_state_ref[...].reshape(1, attn_cols)
    attn_new = KEEP * attn_state + (1.0 - KEEP) * (total[:, cols : cols + attn_cols] / rows_total)
    attn_cols_ref[...] = attn_new.reshape(attn_cols)
    inverse = jnp.broadcast_to(1.0 / cols_new, (SLAB, cols))
    attn_inverse = jnp.concatenate([1.0 / attn_new, jnp.ones((1, 2 * LANES - attn_cols), F32)], axis=1)
    down_inverse = [down(attn_inverse[:, k * LANES : (k + 1) * LANES]) for k in range(2)]

    def step(s, carry):
        g = g_ref[pl.ds(s * SLAB, SLAB), :].astype(F32)
        lane_ref[pl.ds(s * SLAB, SLAB), :] = tiles(g * g * inverse)
        return carry

    lax.fori_loop(0, rows // SLAB, step, 0, unroll=8)
    w_attn = jnp.zeros((8, rows), F32)
    for s in range(attn_cols // SLAB):
        g = ga_ref[pl.ds(s * SLAB, SLAB), :].astype(F32)
        at = s * SLAB
        scale = down_inverse[at // LANES][at % LANES : at % LANES + SLAB]
        w_attn = w_attn + fold(g * g * wide(scale, rows))
    w_attn = jnp.sum(w_attn, axis=0, keepdims=True)
    w_mlp = jnp.concatenate([turned_sum(lane_ref, b * LANES) for b in range(rows // LANES)], axis=1)
    vectors = (row_sums[:, :rows], row_sums[:, rows:], w_mlp, w_attn)
    first = jnp.concatenate([v[:, :half] for v in vectors], axis=1)
    last = jnp.concatenate([v[:, half:] for v in vectors], axis=1)
    early = early_ref.shape[0] // 3
    for at in range(0, early, SLAB):
        p = pa_ref[pl.ds(at, SLAB), :]
        high = p.astype(BF16)
        early_ref[pl.ds(at, SLAB), :] = high
        early_ref[pl.ds(early + at, SLAB), :] = (p - high.astype(F32)).astype(BF16)
    early_ref[pl.ds(2 * early, early), :] = ga_ref[pl.ds(0, early), :]
    kept_ref[...] = jnp.where(core == 0, first, last)
    sent_ref[...] = jnp.where(core == 0, last, first)


def spread_kernel(kept_ref, got_ref, psum_ref, sent_ref):
    value = jnp.concatenate([kept_ref[...] + got_ref[...], psum_ref[...]], axis=1)
    for k in range(sent_ref.shape[0]):
        sent_ref[k] = value


def rows_kernel(widths, got_ref, state_ref, attn_state_ref, sent_ref):
    rows = state_ref.shape[0]
    half = rows // 2
    core = lax.axis_index(CORE)
    total = added(got_ref)
    new, parts = [], []
    for k, (ref, width) in enumerate(zip((state_ref, attn_state_ref), widths)):
        state = ref[...].reshape(1, rows)
        state = jnp.where(core == 0, state[:, :half], state[:, half:])
        new.append(KEEP * state + (1.0 - KEEP) * (total[:, k * half : (k + 1) * half] / width))
        parts.append(tiles(total[:, (2 + k) * half : (3 + k) * half] / new[k]))
    value = jnp.concatenate([*parts, total[:, 4 * half :], *new], axis=1)
    for k in range(sent_ref.shape[0]):
        sent_ref[k] = value


def factor(got_ref, matrix, count):
    total = got_ref[0, :, : 4 * LANES]
    for k in range(1, got_ref.shape[0]):
        total = total + got_ref[k, :, : 4 * LANES]
    q, p = (
        jnp.broadcast_to(jnp.sum(total[:, k * LANES : (k + 1) * LANES], axis=1, keepdims=True), (1, LANES))
        for k in (matrix, 2 + matrix)
    )
    return LEARN_RATE * jnp.sqrt(p / count) / jnp.maximum(1.0, jnp.sqrt(q / count))


def new_rows(got_ref, matrix, half, dx=0):
    row = place(dx, 0)
    at = pl.ds(4 * LANES + matrix * half, half)
    return jnp.concatenate([got_ref[2 * row, :, at], got_ref[2 * row + 1, :, at]], axis=1)


def attn_scales(count, got_ref, attn_cols_ref):
    attn_cols = attn_cols_ref.shape[0]
    across = attn_cols_ref[...].reshape(1, attn_cols)
    across = lax.rsqrt(jnp.concatenate([across, jnp.ones((1, 2 * LANES - attn_cols), F32)], axis=1))
    scale = factor(got_ref, 1, count)
    return [down(across[:, k * LANES : (k + 1) * LANES] * scale) for k in range(2)]


def attn_new(g, p, at, across, along):
    scale = across[at // LANES][at % LANES : at % LANES + SLAB]
    return p - g * wide(scale, g.shape[1]) * along


def attn_kernel(count, got_ref, attn_cols_ref, ga_ref, pa_ref, attn_ref, block_ref, *part_refs):
    attn_cols, rows = ga_ref.shape
    part = attn_cols // len(part_refs)
    across = attn_scales(count, got_ref, attn_cols_ref)
    along = jnp.broadcast_to(lax.rsqrt(new_rows(got_ref, 1, rows // 2)), (SLAB, rows))
    for at in range(0, attn_cols, SLAB):
        rows_at = pl.ds(at, SLAB)
        value = attn_new(ga_ref[rows_at, :].astype(F32), pa_ref[rows_at, :], at, across, along)
        attn_ref[pl.ds(at, SLAB), :] = value
        block_ref[pl.ds(at, SLAB), :] = value.astype(BF16)
        part_refs[at // part][pl.ds(at % part, SLAB), :] = value.astype(BF16)


def early_kernel(count, got_ref, attn_cols_ref, ahead_ref, out_ref):
    early, rows = out_ref.shape
    across = attn_scales(count, got_ref, attn_cols_ref)
    along = jnp.broadcast_to(lax.rsqrt(new_rows(got_ref, 1, rows // 2, 2)), (SLAB, rows))
    for at in range(0, early, SLAB):
        high, low, g = (ahead_ref[pl.ds(k * early + at, SLAB), :].astype(F32) for k in range(3))
        out_ref[pl.ds(at, SLAB), :] = attn_new(g, high + low, at, across, along).astype(BF16)


def place(dx, dy):
    x = lax.rem(lax.axis_index("row_0") + dx, lax.axis_size("row_0"))
    y = lax.rem(lax.axis_index("row_1") + dy, lax.axis_size("row_1"))
    return x * lax.axis_size("row_1") + y


def fill_kernel(offsets, *refs):
    blocks, out_hbm, sems = refs[: len(offsets)], refs[-2], refs[-1]
    width = blocks[0].shape[1]
    copies = []
    for k, (ref, offset) in enumerate(zip(blocks, offsets)):
        dx, dy, first = offset
        at = pl.multiple_of(place(dx, dy) * width, width)
        target = out_hbm.at[pl.ds(first, ref.shape[0]), pl.ds(at, width)]
        copies.append(pltpu.make_async_copy(ref, target, sems.at[k]))
        copies[-1].start()
    for copy in copies:
        copy.wait()


def fill(copy, offsets, blocks):
    count = len(blocks)
    return call(
        functools.partial(fill_kernel, offsets),
        [jax.ShapeDtypeStruct(copy.shape, copy.dtype)],
        (*blocks, copy),
        in_specs=[ON_CHIP] * count + [OFF_CHIP],
        out_specs=[OFF_CHIP],
        scratch=[pltpu.SemaphoreType.DMA((count,))],
        aliases={count: 0},
    )[0]


def finish_kernel(
    count, block_ref, got_ref, cols_ref, attn_cols_ref, attn_ref, g_ref, p_ref,
    copy_hbm, attn_hbm, new_hbm, rows_hbm, cols_hbm, attn_rows_hbm, attn_cols_hbm,
    new_ref, rows_ref, attn_rows_ref, sems,
):
    rows, cols = g_ref.shape
    blocks = rows // LANES
    copies = []

    def put(source, target):
        copies.append(pltpu.make_async_copy(source, target, sems.at[len(copies)]))
        copies[-1].start()

    put(block_ref, copy_hbm.at[:, pl.ds(pl.multiple_of(place(0, 0) * rows, rows), rows)])
    put(attn_ref, attn_hbm)
    put(cols_ref, cols_hbm)
    put(attn_cols_ref, attn_cols_hbm)
    row_factors = new_rows(got_ref, 0, rows // 2)
    rows_ref[...] = row_factors.reshape(rows)
    attn_rows_ref[...] = new_rows(got_ref, 1, rows // 2).reshape(rows)
    along = jnp.broadcast_to(lax.rsqrt(cols_ref[...].reshape(1, cols)), (SLAB, cols))
    scale = factor(got_ref, 0, count)
    row_scale = lax.rsqrt(row_factors)
    for b in range(blocks):
        across = down(row_scale[:, b * LANES : (b + 1) * LANES] * scale)
        for s in range(LANES // SLAB):
            at = pl.ds(b * LANES + s * SLAB, SLAB)
            new_ref[at, :] = (
                p_ref[at, :] - g_ref[at, :].astype(F32) * wide(across[s * SLAB : (s + 1) * SLAB], cols) * along
            )
        at = pl.ds(b * LANES, LANES)
        put(new_ref.at[at], new_hbm.at[at])
    put(rows_ref, rows_hbm)
    put(attn_rows_ref, attn_rows_hbm)
    for copy in copies:
        copy.wait()


def everyone(value, axes):
    return lax.all_to_all(value, axes, 0, 0, tiled=True)


def moved(value, dx, dy):
    xs, ys = lax.axis_size("row_0"), lax.axis_size("row_1")
    pairs = [(x * ys + y, (x + dx) % xs * ys + (y + dy) % ys) for x in range(xs) for y in range(ys)]
    return lax.ppermute(value, ROW, pairs)


def other_core(value):
    return lax.ppermute(value, CORE, [(0, 1), (1, 0)])


def step(
    mlp_param,
    mlp_grad,
    mlp_row_state,
    mlp_col_state,
    attn_param,
    attn_grad,
    attn_row_state,
    attn_col_state,
):
    rows, cols = mlp_grad.shape
    attn_cols = attn_grad.shape[1]
    half = rows // 2
    row_devices, layers = lax.axis_size(ROW), lax.axis_size(LAYERS)
    message = -(-(cols + attn_cols) // LANES) * LANES
    rows_total = rows * row_devices
    widths = (float(cols * lax.axis_size(COL)), float(attn_cols * lax.axis_size(COL)))
    counts = (rows_total * widths[0], rows_total * widths[1])
    attn_grad, attn_param = attn_grad.T, attn_param.T
    blocks = rows // LANES

    sent, row_sums, p_sums, g, ga, p, pa = call(
        sums_kernel,
        [
            pltpu.VMEM((row_devices, 1, message), F32),
            pltpu.VMEM((1, 2 * rows), F32),
            pltpu.VMEM((1, 2 * LANES), F32),
            pltpu.VMEM((rows, cols), BF16),
            pltpu.VMEM((attn_cols, rows), BF16),
            pltpu.VMEM((rows, cols), F32),
            pltpu.VMEM((attn_cols, rows), F32),
        ],
        (mlp_grad, attn_grad, mlp_param, attn_param),
        in_specs=[OFF_CHIP] * 4,
        scratch=[
            pltpu.VMEM((rows + 2 * LANES, LANES), F32),
            pltpu.SemaphoreType.DMA((2 * blocks + 2,)),
        ],
        limit=118 << 19,
    )
    got = everyone(sent, ROW)
    cols_new, attn_cols_new, kept, sent, ahead = call(
        functools.partial(columns_kernel, float(rows_total)),
        [
            pltpu.VMEM((cols,), F32),
            pltpu.VMEM((attn_cols,), F32),
            pltpu.VMEM((1, 4 * half), F32),
            pltpu.VMEM((1, 4 * half), F32),
            pltpu.VMEM((3 * attn_cols, rows), BF16),
        ],
        (got, row_sums, g, ga, pa, mlp_col_state, attn_col_state),
        scratch=[pltpu.VMEM((rows, LANES), F32)],
    )
    swapped = other_core(sent)
    (sent,) = call(
        spread_kernel,
        [pltpu.VMEM((layers, 1, 4 * half + 2 * LANES), F32)],
        (kept, swapped, p_sums),
    )
    got = everyone(sent, LAYERS)
    (sent,) = call(
        functools.partial(rows_kernel, widths),
        [pltpu.VMEM((2 * row_devices, 1, 4 * LANES + 2 * half), F32)],
        (got, mlp_row_state, attn_row_state),
    )
    got = everyone(sent, (*ROW, CORE))
    ahead = moved(ahead, 2, 0)
    attn_new, block, *parts = call(
        functools.partial(attn_kernel, counts[1]),
        [
            pltpu.VMEM((attn_cols, rows), F32),
            pltpu.VMEM((attn_cols, rows), BF16),
            *[pltpu.VMEM((attn_cols // 2, rows), BF16)] * 2,
        ],
        (got, attn_cols_new, ga, pa),
    )
    (across,) = call(
        functools.partial(early_kernel, counts[1]),
        [pltpu.VMEM((attn_cols, rows), BF16)],
        (got, attn_cols_new, ahead),
    )
    partner = moved(parts[0], 0, 1)
    partner_last = moved(parts[1], 0, 1)
    left = moved(block, 1, 0)
    right = moved(block, 3, 0)
    partner_across = moved(across, 0, 1)
    partner_left = moved(partner, 1, 0)
    partner_right = moved(partner, 3, 0)
    last_left = moved(partner_last, 1, 0)
    last_right = moved(partner_last, 3, 0)
    copy, attn_new, mlp_new, rows_new, cols_new, attn_rows_new, attn_cols_new = call(
        functools.partial(finish_kernel, counts[0]),
        [
            jax.ShapeDtypeStruct((attn_cols, rows_total), BF16),
            jax.ShapeDtypeStruct((attn_cols, rows), F32),
            jax.ShapeDtypeStruct((rows, cols), F32),
            jax.ShapeDtypeStruct((rows,), F32),
            jax.ShapeDtypeStruct((cols,), F32),
            jax.ShapeDtypeStruct((rows,), F32),
            jax.ShapeDtypeStruct((attn_cols,), F32),
        ],
        (block, got, cols_new, attn_cols_new, attn_new, g, p),
        out_specs=[OFF_CHIP] * 7,
        scratch=[
            pltpu.VMEM((rows, cols), F32),
            pltpu.VMEM((rows,), F32),
            pltpu.VMEM((rows,), F32),
            pltpu.SemaphoreType.DMA((blocks + 6,)),
        ],
        flops=1 << 22,
    )
    copy = fill(
        copy,
        ((2, 0, 0), (0, 1, 0), (0, 1, attn_cols // 2), (3, 0, 0), (1, 0, 0)),
        (across, partner, partner_last, left, right),
    )
    copy = fill(
        copy,
        ((2, 1, 0), (3, 1, 0), (1, 1, 0), (3, 1, attn_cols // 2), (1, 1, attn_cols // 2)),
        (partner_across, partner_left, partner_right, last_left, last_right),
    )
    return mlp_new, attn_new.T, rows_new, cols_new, attn_rows_new, attn_cols_new, copy.T


def solution(mesh):
    finer = Mesh(mesh.devices.reshape(4, 2, 2, 8, 2), (*ROW, *COL))
    return jax.shard_map(
        step,
        mesh=finer,
        in_specs=(
            P(ROW, COL),
            P(ROW, COL),
            P(ROW),
            P(COL),
            P(ROW, COL),
            P(ROW, COL),
            P(ROW),
            P(COL),
        ),
        out_specs=(P(ROW, COL), P(ROW, COL), P(ROW), P(COL), P(ROW), P(COL), P(None, COL)),
        check_vma=False,
    )
```

```python
import functools

import jax
import jax.numpy as jnp
from jax import lax
from jax.experimental import pallas as pl
from jax.experimental.pallas import tpu as pltpu
from jax.sharding import Mesh
from jax.sharding import PartitionSpec as P

STEP = 4
ROW = ("row_0", "row_1")
COL = ("col_0", "col_1", "col_2")
Y_HI, Z, CORE = COL
LAYERS = (Y_HI, Z)

TINY_SQUARE = 1e-30
LEARN_RATE = 0.05
DECAY_POWER = 0.8
KEEP = 1.0 - STEP ** (-DECAY_POWER)

F32, BF16 = jnp.float32, jnp.bfloat16
SLAB = 16
LANES = 128
ON_CHIP = pl.BlockSpec(memory_space=pltpu.VMEM)
OFF_CHIP = pl.BlockSpec(memory_space=pltpu.HBM)


def call(kernel, outs, args, in_specs=None, out_specs=None, scratch=(), limit=4 << 20, aliases=None, flops=0):
    return pl.pallas_call(
        kernel,
        out_shape=outs,
        in_specs=in_specs or [ON_CHIP] * len(args),
        out_specs=out_specs or [ON_CHIP] * len(outs),
        scratch_shapes=scratch,
        input_output_aliases=aliases or {},
        cost_estimate=pl.CostEstimate(flops=flops, bytes_accessed=flops, transcendentals=0) if flops else None,
        compiler_params=pltpu.CompilerParams(vmem_limit_bytes=limit),
    )(*args)


def tiles(value):
    width = value.shape[1] // LANES
    return sum((value[:, k * LANES : (k + 1) * LANES] for k in range(1, width)), value[:, :LANES])


def wide(value, width):
    return jnp.concatenate([value] * (width // LANES), axis=1)


def turned_sum(ref, start):
    return jnp.sum(ref[pl.ds(start, LANES), :].T, axis=0, keepdims=True)


def down(value):
    return jnp.broadcast_to(value, (LANES, LANES)).T


def fold(value):
    return value[:8] + value[8:]


def added(ref):
    total = ref[0]
    for k in range(1, ref.shape[0]):
        total = total + ref[k]
    return total


def sums_kernel(
    g_hbm, ga_hbm, p_hbm, pa_hbm, sent_ref, rows_ref, psum_ref, g_ref, ga_ref, p_ref, pa_ref, lane_ref, sems
):
    rows, cols = g_hbm.shape
    attn_cols = ga_hbm.shape[0]
    blocks = rows // LANES
    g_copies = [
        pltpu.make_async_copy(g_hbm.at[pl.ds(b * LANES, LANES)], g_ref.at[pl.ds(b * LANES, LANES)], sems.at[b])
        for b in range(blocks)
    ]
    p_copies = [
        pltpu.make_async_copy(
            p_hbm.at[pl.ds(b * LANES, LANES)], p_ref.at[pl.ds(b * LANES, LANES)], sems.at[blocks + b]
        )
        for b in range(blocks)
    ]
    ga_copy = pltpu.make_async_copy(ga_hbm, ga_ref, sems.at[2 * blocks])
    pa_copy = pltpu.make_async_copy(pa_hbm, pa_ref, sems.at[2 * blocks + 1])
    for copy in (ga_copy, *g_copies, *p_copies, pa_copy):
        copy.start()
    lane_ref[pl.ds(rows, 2 * LANES), :] = jnp.zeros((2 * LANES, LANES), F32)

    def squares(ref, start, first):
        def step(s, acc):
            g = ref[pl.ds(start + s * SLAB, SLAB), :].astype(F32)
            g = g * g
            lane_ref[pl.ds(first + start + s * SLAB, SLAB), :] = tiles(g)
            return acc + fold(g)

        return step

    def own_squares(ref, start):
        def step(s, acc):
            p = ref[pl.ds(start + s * SLAB, SLAB), :]
            return acc + fold(p * p)

        return step

    eight = jnp.zeros((8, cols), F32)
    ga_copy.wait()
    row_sum = lax.fori_loop(0, attn_cols // SLAB, squares(ga_ref, 0, rows), jnp.zeros((8, rows), F32), unroll=4)
    rows_ref[:, pl.ds(rows, rows)] = jnp.sum(row_sum, axis=0, keepdims=True)
    steps = LANES // SLAB
    col_sum = eight
    for b, copy in enumerate(g_copies):
        copy.wait()
        col_sum = lax.fori_loop(0, steps, squares(g_ref, b * LANES, 0), col_sum, unroll=True)
        rows_ref[:, pl.ds(b * LANES, LANES)] = turned_sum(lane_ref, b * LANES)
    rows_ref[...] += jnp.concatenate(
        [jnp.full((1, rows), cols * TINY_SQUARE, F32), jnp.full((1, rows), attn_cols * TINY_SQUARE, F32)], axis=1
    )
    col_sums = jnp.concatenate(
        [
            jnp.sum(col_sum, axis=0, keepdims=True),
            turned_sum(lane_ref, rows),
            turned_sum(lane_ref, rows + LANES),
        ],
        axis=1,
    ) + rows * TINY_SQUARE
    for k in range(sent_ref.shape[0]):
        sent_ref[k] = col_sums
    p_sum = eight
    for b, copy in enumerate(p_copies):
        copy.wait()
        p_sum = lax.fori_loop(0, steps, own_squares(p_ref, b * LANES), p_sum, unroll=True)
    pa_copy.wait()
    pa_sum = lax.fori_loop(0, attn_cols // SLAB, own_squares(pa_ref, 0), jnp.zeros((8, rows), F32), unroll=4)
    psum_ref[:, :LANES] = jnp.sum(tiles(p_sum), axis=0, keepdims=True)
    psum_ref[:, LANES:] = jnp.sum(tiles(pa_sum), axis=0, keepdims=True)


def columns_kernel(
    rows_total, got_ref, rows_ref, g_ref, ga_ref, pa_ref, state_ref, attn_state_ref,
    cols_ref, attn_cols_ref, kept_ref, sent_ref, early_ref, lane_ref,
):
    rows, cols = g_ref.shape
    attn_cols = ga_ref.shape[0]
    half = rows // 2
    core = lax.axis_index(CORE)
    total = added(got_ref)
    row_sums = rows_ref[...]
    cols_new = KEEP * state_ref[...].reshape(1, cols) + (1.0 - KEEP) * (total[:, :cols] / rows_total)
    cols_ref[...] = cols_new.reshape(cols)
    attn_state = attn_state_ref[...].reshape(1, attn_cols)
    attn_new = KEEP * attn_state + (1.0 - KEEP) * (total[:, cols : cols + attn_cols] / rows_total)
    attn_cols_ref[...] = attn_new.reshape(attn_cols)
    inverse = jnp.broadcast_to(1.0 / cols_new, (SLAB, cols))
    attn_inverse = jnp.concatenate([1.0 / attn_new, jnp.ones((1, 2 * LANES - attn_cols), F32)], axis=1)
    down_inverse = [down(attn_inverse[:, k * LANES : (k + 1) * LANES]) for k in range(2)]

    def step(s, carry):
        g = g_ref[pl.ds(s * SLAB, SLAB), :].astype(F32)
        lane_ref[pl.ds(s * SLAB, SLAB), :] = tiles(g * g * inverse)
        return carry

    lax.fori_loop(0, rows // SLAB, step, 0, unroll=8)
    w_attn = jnp.zeros((8, rows), F32)
    for s in range(attn_cols // SLAB):
        g = ga_ref[pl.ds(s * SLAB, SLAB), :].astype(F32)
        at = s * SLAB
        scale = down_inverse[at // LANES][at % LANES : at % LANES + SLAB]
        w_attn = w_attn + fold(g * g * wide(scale, rows))
    w_attn = jnp.sum(w_attn, axis=0, keepdims=True)
    w_mlp = jnp.concatenate([turned_sum(lane_ref, b * LANES) for b in range(rows // LANES)], axis=1)
    vectors = (row_sums[:, :rows], row_sums[:, rows:], w_mlp, w_attn)
    first = jnp.concatenate([v[:, :half] for v in vectors], axis=1)
    last = jnp.concatenate([v[:, half:] for v in vectors], axis=1)
    early = early_ref.shape[0] // 3
    for at in range(0, early, SLAB):
        p = pa_ref[pl.ds(at, SLAB), :]
        high = p.astype(BF16)
        early_ref[pl.ds(at, SLAB), :] = high
        early_ref[pl.ds(early + at, SLAB), :] = (p - high.astype(F32)).astype(BF16)
    early_ref[pl.ds(2 * early, early), :] = ga_ref[pl.ds(0, early), :]
    kept_ref[...] = jnp.where(core == 0, first, last)
    sent_ref[...] = jnp.where(core == 0, last, first)


def spread_kernel(kept_ref, got_ref, psum_ref, sent_ref):
    value = jnp.concatenate([kept_ref[...] + got_ref[...], psum_ref[...]], axis=1)
    for k in range(sent_ref.shape[0]):
        sent_ref[k] = value


def rows_kernel(widths, got_ref, state_ref, attn_state_ref, sent_ref):
    rows = state_ref.shape[0]
    half = rows // 2
    core = lax.axis_index(CORE)
    total = added(got_ref)
    new, parts = [], []
    for k, (ref, width) in enumerate(zip((state_ref, attn_state_ref), widths)):
        state = ref[...].reshape(1, rows)
        state = jnp.where(core == 0, state[:, :half], state[:, half:])
        new.append(KEEP * state + (1.0 - KEEP) * (total[:, k * half : (k + 1) * half] / width))
        parts.append(tiles(total[:, (2 + k) * half : (3 + k) * half] / new[k]))
    value = jnp.concatenate([*parts, total[:, 4 * half :], *new], axis=1)
    for k in range(sent_ref.shape[0]):
        sent_ref[k] = value


def factor(got_ref, matrix, count):
    total = got_ref[0, :, : 4 * LANES]
    for k in range(1, got_ref.shape[0]):
        total = total + got_ref[k, :, : 4 * LANES]
    q, p = (
        jnp.broadcast_to(jnp.sum(total[:, k * LANES : (k + 1) * LANES], axis=1, keepdims=True), (1, LANES))
        for k in (matrix, 2 + matrix)
    )
    return LEARN_RATE * jnp.sqrt(p / count) / jnp.maximum(1.0, jnp.sqrt(q / count))


def new_rows(got_ref, matrix, half, dx=0):
    row = place(dx, 0)
    at = pl.ds(4 * LANES + matrix * half, half)
    return jnp.concatenate([got_ref[2 * row, :, at], got_ref[2 * row + 1, :, at]], axis=1)


def attn_scales(count, got_ref, attn_cols_ref):
    attn_cols = attn_cols_ref.shape[0]
    across = attn_cols_ref[...].reshape(1, attn_cols)
    across = lax.rsqrt(jnp.concatenate([across, jnp.ones((1, 2 * LANES - attn_cols), F32)], axis=1))
    scale = factor(got_ref, 1, count)
    return [down(across[:, k * LANES : (k + 1) * LANES] * scale) for k in range(2)]


def attn_new(g, p, at, across, along):
    scale = across[at // LANES][at % LANES : at % LANES + SLAB]
    return p - g * wide(scale, g.shape[1]) * along


def attn_kernel(count, got_ref, attn_cols_ref, ga_ref, pa_ref, attn_ref, block_ref, *part_refs):
    attn_cols, rows = ga_ref.shape
    part = attn_cols // len(part_refs)
    across = attn_scales(count, got_ref, attn_cols_ref)
    along = jnp.broadcast_to(lax.rsqrt(new_rows(got_ref, 1, rows // 2)), (SLAB, rows))
    for at in range(0, attn_cols, SLAB):
        rows_at = pl.ds(at, SLAB)
        value = attn_new(ga_ref[rows_at, :].astype(F32), pa_ref[rows_at, :], at, across, along)
        attn_ref[pl.ds(at, SLAB), :] = value
        block_ref[pl.ds(at, SLAB), :] = value.astype(BF16)
        part_refs[at // part][pl.ds(at % part, SLAB), :] = value.astype(BF16)


def early_kernel(count, got_ref, attn_cols_ref, ahead_ref, out_ref):
    early, rows = out_ref.shape
    across = attn_scales(count, got_ref, attn_cols_ref)
    along = jnp.broadcast_to(lax.rsqrt(new_rows(got_ref, 1, rows // 2, 2)), (SLAB, rows))
    for at in range(0, early, SLAB):
        high, low, g = (ahead_ref[pl.ds(k * early + at, SLAB), :].astype(F32) for k in range(3))
        out_ref[pl.ds(at, SLAB), :] = attn_new(g, high + low, at, across, along).astype(BF16)


NEAR, FAR = "near", "far"


def place(dx, dy):
    x = lax.axis_index("row_0")
    if dx == NEAR:
        dx = 1 + 2 * lax.rem(x, 2)
    elif dx == FAR:
        dx = 3 - 2 * lax.rem(x, 2)
    x = lax.rem(x + dx, lax.axis_size("row_0"))
    y = lax.rem(lax.axis_index("row_1") + dy, lax.axis_size("row_1"))
    return x * lax.axis_size("row_1") + y


def fill_kernel(offsets, *refs):
    blocks, out_hbm, sems = refs[: len(offsets)], refs[-2], refs[-1]
    width = blocks[0].shape[1]
    copies = []
    for k, (ref, offset) in enumerate(zip(blocks, offsets)):
        dx, dy, first = offset
        at = pl.multiple_of(place(dx, dy) * width, width)
        target = out_hbm.at[pl.ds(first, ref.shape[0]), pl.ds(at, width)]
        copies.append(pltpu.make_async_copy(ref, target, sems.at[k]))
        copies[-1].start()
    for copy in copies:
        copy.wait()


def fill(copy, offsets, blocks):
    count = len(blocks)
    return call(
        functools.partial(fill_kernel, offsets),
        [jax.ShapeDtypeStruct(copy.shape, copy.dtype)],
        (*blocks, copy),
        in_specs=[ON_CHIP] * count + [OFF_CHIP],
        out_specs=[OFF_CHIP],
        scratch=[pltpu.SemaphoreType.DMA((count,))],
        aliases={count: 0},
    )[0]


def finish_kernel(
    count, block_ref, got_ref, cols_ref, attn_cols_ref, attn_ref, g_ref, p_ref,
    copy_hbm, attn_hbm, new_hbm, rows_hbm, cols_hbm, attn_rows_hbm, attn_cols_hbm,
    new_ref, rows_ref, attn_rows_ref, sems,
):
    rows, cols = g_ref.shape
    blocks = rows // LANES
    copies = []

    def put(source, target):
        copies.append(pltpu.make_async_copy(source, target, sems.at[len(copies)]))
        copies[-1].start()

    put(block_ref, copy_hbm.at[:, pl.ds(pl.multiple_of(place(0, 0) * rows, rows), rows)])
    put(attn_ref, attn_hbm)
    put(cols_ref, cols_hbm)
    put(attn_cols_ref, attn_cols_hbm)
    row_factors = new_rows(got_ref, 0, rows // 2)
    rows_ref[...] = row_factors.reshape(rows)
    attn_rows_ref[...] = new_rows(got_ref, 1, rows // 2).reshape(rows)
    along = jnp.broadcast_to(lax.rsqrt(cols_ref[...].reshape(1, cols)), (SLAB, cols))
    scale = factor(got_ref, 0, count)
    row_scale = lax.rsqrt(row_factors)
    for b in range(blocks):
        across = down(row_scale[:, b * LANES : (b + 1) * LANES] * scale)
        for s in range(LANES // SLAB):
            at = pl.ds(b * LANES + s * SLAB, SLAB)
            new_ref[at, :] = (
                p_ref[at, :] - g_ref[at, :].astype(F32) * wide(across[s * SLAB : (s + 1) * SLAB], cols) * along
            )
        at = pl.ds(b * LANES, LANES)
        put(new_ref.at[at], new_hbm.at[at])
    put(rows_ref, rows_hbm)
    put(attn_rows_ref, attn_rows_hbm)
    for copy in copies:
        copy.wait()


def everyone(value, axes):
    return lax.all_to_all(value, axes, 0, 0, tiled=True)


def moved(value, dx, dy):
    xs, ys = lax.axis_size("row_0"), lax.axis_size("row_1")
    steps = {NEAR: (1, xs - 1), FAR: (xs - 1, 1)}.get(dx, (dx, dx))
    pairs = [(x * ys + y, (x + steps[x % 2]) % xs * ys + (y + dy) % ys) for x in range(xs) for y in range(ys)]
    return lax.ppermute(value, ROW, pairs)


def other_core(value):
    return lax.ppermute(value, CORE, [(0, 1), (1, 0)])


def step(
    mlp_param,
    mlp_grad,
    mlp_row_state,
    mlp_col_state,
    attn_param,
    attn_grad,
    attn_row_state,
    attn_col_state,
):
    rows, cols = mlp_grad.shape
    attn_cols = attn_grad.shape[1]
    half = rows // 2
    row_devices, layers = lax.axis_size(ROW), lax.axis_size(LAYERS)
    message = -(-(cols + attn_cols) // LANES) * LANES
    rows_total = rows * row_devices
    widths = (float(cols * lax.axis_size(COL)), float(attn_cols * lax.axis_size(COL)))
    counts = (rows_total * widths[0], rows_total * widths[1])
    attn_grad, attn_param = attn_grad.T, attn_param.T
    blocks = rows // LANES

    sent, row_sums, p_sums, g, ga, p, pa = call(
        sums_kernel,
        [
            pltpu.VMEM((row_devices, 1, message), F32),
            pltpu.VMEM((1, 2 * rows), F32),
            pltpu.VMEM((1, 2 * LANES), F32),
            pltpu.VMEM((rows, cols), BF16),
            pltpu.VMEM((attn_cols, rows), BF16),
            pltpu.VMEM((rows, cols), F32),
            pltpu.VMEM((attn_cols, rows), F32),
        ],
        (mlp_grad, attn_grad, mlp_param, attn_param),
        in_specs=[OFF_CHIP] * 4,
        scratch=[
            pltpu.VMEM((rows + 2 * LANES, LANES), F32),
            pltpu.SemaphoreType.DMA((2 * blocks + 2,)),
        ],
        limit=118 << 19,
    )
    got = everyone(sent, ROW)
    cols_new, attn_cols_new, kept, sent, ahead = call(
        functools.partial(columns_kernel, float(rows_total)),
        [
            pltpu.VMEM((cols,), F32),
            pltpu.VMEM((attn_cols,), F32),
            pltpu.VMEM((1, 4 * half), F32),
            pltpu.VMEM((1, 4 * half), F32),
            pltpu.VMEM((3 * attn_cols, rows), BF16),
        ],
        (got, row_sums, g, ga, pa, mlp_col_state, attn_col_state),
        scratch=[pltpu.VMEM((rows, LANES), F32)],
    )
    swapped = other_core(sent)
    (sent,) = call(
        spread_kernel,
        [pltpu.VMEM((layers, 1, 4 * half + 2 * LANES), F32)],
        (kept, swapped, p_sums),
    )
    got = everyone(sent, LAYERS)
    (sent,) = call(
        functools.partial(rows_kernel, widths),
        [pltpu.VMEM((2 * row_devices, 1, 4 * LANES + 2 * half), F32)],
        (got, mlp_row_state, attn_row_state),
    )
    got = everyone(sent, (*ROW, CORE))
    ahead = moved(ahead, 2, 0)
    attn_new, block, *parts = call(
        functools.partial(attn_kernel, counts[1]),
        [
            pltpu.VMEM((attn_cols, rows), F32),
            pltpu.VMEM((attn_cols, rows), BF16),
            *[pltpu.VMEM((attn_cols // 2, rows), BF16)] * 2,
        ],
        (got, attn_cols_new, ga, pa),
    )
    (across,) = call(
        functools.partial(early_kernel, counts[1]),
        [pltpu.VMEM((attn_cols, rows), BF16)],
        (got, attn_cols_new, ahead),
    )
    partner = moved(parts[0], 0, 1)
    partner_last = moved(parts[1], 0, 1)
    near = moved(block, NEAR, 0)
    far = moved(block, FAR, 0)
    partner_across = moved(across, 0, 1)
    partner_near = moved(partner, NEAR, 0)
    partner_far = moved(partner, FAR, 0)
    last_near = moved(partner_last, NEAR, 0)
    last_far = moved(partner_last, FAR, 0)
    copy, attn_new, mlp_new, rows_new, cols_new, attn_rows_new, attn_cols_new = call(
        functools.partial(finish_kernel, counts[0]),
        [
            jax.ShapeDtypeStruct((attn_cols, rows_total), BF16),
            jax.ShapeDtypeStruct((attn_cols, rows), F32),
            jax.ShapeDtypeStruct((rows, cols), F32),
            jax.ShapeDtypeStruct((rows,), F32),
            jax.ShapeDtypeStruct((cols,), F32),
            jax.ShapeDtypeStruct((rows,), F32),
            jax.ShapeDtypeStruct((attn_cols,), F32),
        ],
        (block, got, cols_new, attn_cols_new, attn_new, g, p),
        out_specs=[OFF_CHIP] * 7,
        scratch=[
            pltpu.VMEM((rows, cols), F32),
            pltpu.VMEM((rows,), F32),
            pltpu.VMEM((rows,), F32),
            pltpu.SemaphoreType.DMA((blocks + 6,)),
        ],
        flops=1 << 22,
    )
    copy = fill(
        copy,
        ((2, 0, 0), (0, 1, 0), (0, 1, attn_cols // 2), (NEAR, 0, 0), (FAR, 0, 0)),
        (across, partner, partner_last, near, far),
    )
    copy = fill(
        copy,
        ((2, 1, 0), (NEAR, 1, 0), (FAR, 1, 0), (NEAR, 1, attn_cols // 2), (FAR, 1, attn_cols // 2)),
        (partner_across, partner_near, partner_far, last_near, last_far),
    )
    return mlp_new, attn_new.T, rows_new, cols_new, attn_rows_new, attn_cols_new, copy.T


def solution(mesh):
    finer = Mesh(mesh.devices.reshape(4, 2, 2, 8, 2), (*ROW, *COL))
    return jax.shard_map(
        step,
        mesh=finer,
        in_specs=(
            P(ROW, COL),
            P(ROW, COL),
            P(ROW),
            P(COL),
            P(ROW, COL),
            P(ROW, COL),
            P(ROW),
            P(COL),
        ),
        out_specs=(P(ROW, COL), P(ROW, COL), P(ROW), P(COL), P(ROW), P(COL), P(None, COL)),
        check_vma=False,
    )
```

```python
import functools

import jax
import jax.numpy as jnp
from jax import lax
from jax.experimental import pallas as pl
from jax.experimental.pallas import tpu as pltpu
from jax.sharding import Mesh
from jax.sharding import PartitionSpec as P

STEP = 4
ROW = ("row_0", "row_1")
COL = ("col_0", "col_1", "col_2")
Y_HI, Z, CORE = COL
LAYERS = (Y_HI, Z)

TINY_SQUARE = 1e-30
LEARN_RATE = 0.05
DECAY_POWER = 0.8
KEEP = 1.0 - STEP ** (-DECAY_POWER)

F32, BF16 = jnp.float32, jnp.bfloat16
SLAB = 16
LANES = 128
ON_CHIP = pl.BlockSpec(memory_space=pltpu.VMEM)
OFF_CHIP = pl.BlockSpec(memory_space=pltpu.HBM)


def call(kernel, outs, args, in_specs=None, out_specs=None, scratch=(), limit=4 << 20, aliases=None, flops=0):
    return pl.pallas_call(
        kernel,
        out_shape=outs,
        in_specs=in_specs or [ON_CHIP] * len(args),
        out_specs=out_specs or [ON_CHIP] * len(outs),
        scratch_shapes=scratch,
        input_output_aliases=aliases or {},
        cost_estimate=pl.CostEstimate(flops=flops, bytes_accessed=flops, transcendentals=0) if flops else None,
        compiler_params=pltpu.CompilerParams(vmem_limit_bytes=limit),
    )(*args)


def tiles(value):
    width = value.shape[1] // LANES
    return sum((value[:, k * LANES : (k + 1) * LANES] for k in range(1, width)), value[:, :LANES])


def wide(value, width):
    return jnp.concatenate([value] * (width // LANES), axis=1)


def turned_sum(ref, start):
    return jnp.sum(ref[pl.ds(start, LANES), :].T, axis=0, keepdims=True)


def down(value):
    return jnp.broadcast_to(value, (LANES, LANES)).T


def fold(value):
    return value[:8] + value[8:]


def added(ref):
    total = ref[0]
    for k in range(1, ref.shape[0]):
        total = total + ref[k]
    return total


def sums_kernel(
    g_hbm, ga_hbm, p_hbm, pa_hbm, sent_ref, rows_ref, psum_ref, g_ref, ga_ref, p_ref, pa_ref, lane_ref, sems
):
    rows, cols = g_hbm.shape
    attn_cols = ga_hbm.shape[0]
    blocks = rows // LANES
    g_copies = [
        pltpu.make_async_copy(g_hbm.at[pl.ds(b * LANES, LANES)], g_ref.at[pl.ds(b * LANES, LANES)], sems.at[b])
        for b in range(blocks)
    ]
    p_copies = [
        pltpu.make_async_copy(
            p_hbm.at[pl.ds(b * LANES, LANES)], p_ref.at[pl.ds(b * LANES, LANES)], sems.at[blocks + b]
        )
        for b in range(blocks)
    ]
    ga_copy = pltpu.make_async_copy(ga_hbm, ga_ref, sems.at[2 * blocks])
    pa_copy = pltpu.make_async_copy(pa_hbm, pa_ref, sems.at[2 * blocks + 1])
    for copy in (ga_copy, *g_copies, *p_copies, pa_copy):
        copy.start()
    lane_ref[pl.ds(rows, 2 * LANES), :] = jnp.zeros((2 * LANES, LANES), F32)

    def squares(ref, start, first):
        def step(s, acc):
            g = ref[pl.ds(start + s * SLAB, SLAB), :].astype(F32)
            g = g * g
            lane_ref[pl.ds(first + start + s * SLAB, SLAB), :] = tiles(g)
            return acc + fold(g)

        return step

    def own_squares(ref, start):
        def step(s, acc):
            p = ref[pl.ds(start + s * SLAB, SLAB), :]
            return acc + fold(p * p)

        return step

    eight = jnp.zeros((8, cols), F32)
    ga_copy.wait()
    row_sum = lax.fori_loop(0, attn_cols // SLAB, squares(ga_ref, 0, rows), jnp.zeros((8, rows), F32), unroll=4)
    rows_ref[:, pl.ds(rows, rows)] = jnp.sum(row_sum, axis=0, keepdims=True)
    steps = LANES // SLAB
    col_sum = eight
    for b, copy in enumerate(g_copies):
        copy.wait()
        col_sum = lax.fori_loop(0, steps, squares(g_ref, b * LANES, 0), col_sum, unroll=True)
        rows_ref[:, pl.ds(b * LANES, LANES)] = turned_sum(lane_ref, b * LANES)
    rows_ref[...] += jnp.concatenate(
        [jnp.full((1, rows), cols * TINY_SQUARE, F32), jnp.full((1, rows), attn_cols * TINY_SQUARE, F32)], axis=1
    )
    col_sums = jnp.concatenate(
        [
            jnp.sum(col_sum, axis=0, keepdims=True),
            turned_sum(lane_ref, rows),
            turned_sum(lane_ref, rows + LANES),
        ],
        axis=1,
    ) + rows * TINY_SQUARE
    for k in range(sent_ref.shape[0]):
        sent_ref[k] = col_sums
    p_sum = eight
    for b, copy in enumerate(p_copies):
        copy.wait()
        p_sum = lax.fori_loop(0, steps, own_squares(p_ref, b * LANES), p_sum, unroll=True)
    pa_copy.wait()
    pa_sum = lax.fori_loop(0, attn_cols // SLAB, own_squares(pa_ref, 0), jnp.zeros((8, rows), F32), unroll=4)
    psum_ref[:, :LANES] = jnp.sum(tiles(p_sum), axis=0, keepdims=True)
    psum_ref[:, LANES:] = jnp.sum(tiles(pa_sum), axis=0, keepdims=True)


def columns_kernel(
    rows_total, got_ref, rows_ref, g_ref, ga_ref, pa_ref, state_ref, attn_state_ref,
    cols_ref, attn_cols_ref, kept_ref, sent_ref, early_ref, lane_ref,
):
    rows, cols = g_ref.shape
    attn_cols = ga_ref.shape[0]
    half = rows // 2
    core = lax.axis_index(CORE)
    total = added(got_ref)
    row_sums = rows_ref[...]
    cols_new = KEEP * state_ref[...].reshape(1, cols) + (1.0 - KEEP) * (total[:, :cols] / rows_total)
    cols_ref[...] = cols_new.reshape(cols)
    attn_state = attn_state_ref[...].reshape(1, attn_cols)
    attn_new = KEEP * attn_state + (1.0 - KEEP) * (total[:, cols : cols + attn_cols] / rows_total)
    attn_cols_ref[...] = attn_new.reshape(attn_cols)
    inverse = jnp.broadcast_to(1.0 / cols_new, (SLAB, cols))
    attn_inverse = jnp.concatenate([1.0 / attn_new, jnp.ones((1, 2 * LANES - attn_cols), F32)], axis=1)
    down_inverse = [down(attn_inverse[:, k * LANES : (k + 1) * LANES]) for k in range(2)]

    def step(s, carry):
        g = g_ref[pl.ds(s * SLAB, SLAB), :].astype(F32)
        lane_ref[pl.ds(s * SLAB, SLAB), :] = tiles(g * g * inverse)
        return carry

    lax.fori_loop(0, rows // SLAB, step, 0, unroll=8)
    w_attn = jnp.zeros((8, rows), F32)
    for s in range(attn_cols // SLAB):
        g = ga_ref[pl.ds(s * SLAB, SLAB), :].astype(F32)
        at = s * SLAB
        scale = down_inverse[at // LANES][at % LANES : at % LANES + SLAB]
        w_attn = w_attn + fold(g * g * wide(scale, rows))
    w_attn = jnp.sum(w_attn, axis=0, keepdims=True)
    w_mlp = jnp.concatenate([turned_sum(lane_ref, b * LANES) for b in range(rows // LANES)], axis=1)
    vectors = (row_sums[:, :rows], row_sums[:, rows:], w_mlp, w_attn)
    first = jnp.concatenate([v[:, :half] for v in vectors], axis=1)
    last = jnp.concatenate([v[:, half:] for v in vectors], axis=1)
    early = early_ref.shape[0] // 3
    for at in range(0, early, SLAB):
        p = pa_ref[pl.ds(at, SLAB), :]
        high = p.astype(BF16)
        early_ref[pl.ds(at, SLAB), :] = high
        early_ref[pl.ds(early + at, SLAB), :] = (p - high.astype(F32)).astype(BF16)
    early_ref[pl.ds(2 * early, early), :] = ga_ref[pl.ds(0, early), :]
    kept_ref[...] = jnp.where(core == 0, first, last)
    sent_ref[...] = jnp.where(core == 0, last, first)


def spread_kernel(kept_ref, got_ref, psum_ref, sent_ref):
    value = jnp.concatenate([kept_ref[...] + got_ref[...], psum_ref[...]], axis=1)
    for k in range(sent_ref.shape[0]):
        sent_ref[k] = value


def rows_kernel(widths, got_ref, state_ref, attn_state_ref, sent_ref):
    rows = state_ref.shape[0]
    half = rows // 2
    core = lax.axis_index(CORE)
    total = added(got_ref)
    new, parts = [], []
    for k, (ref, width) in enumerate(zip((state_ref, attn_state_ref), widths)):
        state = ref[...].reshape(1, rows)
        state = jnp.where(core == 0, state[:, :half], state[:, half:])
        new.append(KEEP * state + (1.0 - KEEP) * (total[:, k * half : (k + 1) * half] / width))
        parts.append(tiles(total[:, (2 + k) * half : (3 + k) * half] / new[k]))
    value = jnp.concatenate([*parts, total[:, 4 * half :], *new], axis=1)
    for k in range(sent_ref.shape[0]):
        sent_ref[k] = value


def factor(got_ref, matrix, count):
    total = got_ref[0, :, : 4 * LANES]
    for k in range(1, got_ref.shape[0]):
        total = total + got_ref[k, :, : 4 * LANES]
    q, p = (
        jnp.broadcast_to(jnp.sum(total[:, k * LANES : (k + 1) * LANES], axis=1, keepdims=True), (1, LANES))
        for k in (matrix, 2 + matrix)
    )
    return LEARN_RATE * jnp.sqrt(p / count) / jnp.maximum(1.0, jnp.sqrt(q / count))


def new_rows(got_ref, matrix, half, dx=0):
    row = place(dx, 0)
    at = pl.ds(4 * LANES + matrix * half, half)
    return jnp.concatenate([got_ref[2 * row, :, at], got_ref[2 * row + 1, :, at]], axis=1)


def attn_scales(count, got_ref, attn_cols_ref):
    attn_cols = attn_cols_ref.shape[0]
    across = attn_cols_ref[...].reshape(1, attn_cols)
    across = lax.rsqrt(jnp.concatenate([across, jnp.ones((1, 2 * LANES - attn_cols), F32)], axis=1))
    scale = factor(got_ref, 1, count)
    return [down(across[:, k * LANES : (k + 1) * LANES] * scale) for k in range(2)]


def attn_new(g, p, at, across, along):
    scale = across[at // LANES][at % LANES : at % LANES + SLAB]
    return p - g * wide(scale, g.shape[1]) * along


def attn_kernel(count, got_ref, attn_cols_ref, ga_ref, pa_ref, attn_ref, block_ref, *part_refs):
    attn_cols, rows = ga_ref.shape
    part = attn_cols // len(part_refs)
    across = attn_scales(count, got_ref, attn_cols_ref)
    along = jnp.broadcast_to(lax.rsqrt(new_rows(got_ref, 1, rows // 2)), (SLAB, rows))
    for at in range(0, attn_cols, SLAB):
        rows_at = pl.ds(at, SLAB)
        value = attn_new(ga_ref[rows_at, :].astype(F32), pa_ref[rows_at, :], at, across, along)
        attn_ref[pl.ds(at, SLAB), :] = value
        block_ref[pl.ds(at, SLAB), :] = value.astype(BF16)
        part_refs[at // part][pl.ds(at % part, SLAB), :] = value.astype(BF16)


def early_kernel(count, got_ref, attn_cols_ref, ahead_ref, out_ref):
    early, rows = out_ref.shape
    across = attn_scales(count, got_ref, attn_cols_ref)
    along = jnp.broadcast_to(lax.rsqrt(new_rows(got_ref, 1, rows // 2, 2)), (SLAB, rows))
    for at in range(0, early, SLAB):
        high, low, g = (ahead_ref[pl.ds(k * early + at, SLAB), :].astype(F32) for k in range(3))
        out_ref[pl.ds(at, SLAB), :] = attn_new(g, high + low, at, across, along).astype(BF16)


NEAR, FAR = "near", "far"


def place(dx, dy):
    x = lax.axis_index("row_0")
    if dx == NEAR:
        dx = 1 + 2 * lax.rem(x, 2)
    elif dx == FAR:
        dx = 3 - 2 * lax.rem(x, 2)
    x = lax.rem(x + dx, lax.axis_size("row_0"))
    y = lax.rem(lax.axis_index("row_1") + dy, lax.axis_size("row_1"))
    return x * lax.axis_size("row_1") + y


def fill_kernel(offsets, *refs):
    blocks, out_hbm, sems = refs[: len(offsets)], refs[-2], refs[-1]
    width = blocks[0].shape[1]
    copies = []
    for k, (ref, offset) in enumerate(zip(blocks, offsets)):
        dx, dy, first = offset
        at = pl.multiple_of(place(dx, dy) * width, width)
        target = out_hbm.at[pl.ds(first, ref.shape[0]), pl.ds(at, width)]
        copies.append(pltpu.make_async_copy(ref, target, sems.at[k]))
        copies[-1].start()
    for copy in copies:
        copy.wait()


def fill(copy, offsets, blocks):
    count = len(blocks)
    return call(
        functools.partial(fill_kernel, offsets),
        [jax.ShapeDtypeStruct(copy.shape, copy.dtype)],
        (*blocks, copy),
        in_specs=[ON_CHIP] * count + [OFF_CHIP],
        out_specs=[OFF_CHIP],
        scratch=[pltpu.SemaphoreType.DMA((count,))],
        aliases={count: 0},
    )[0]


def finish_kernel(
    count, block_ref, got_ref, cols_ref, attn_cols_ref, attn_ref, g_ref, p_ref,
    copy_hbm, attn_hbm, new_hbm, rows_hbm, cols_hbm, attn_rows_hbm, attn_cols_hbm,
    new_ref, rows_ref, attn_rows_ref, sems,
):
    rows, cols = g_ref.shape
    blocks = rows // LANES
    copies = []

    def put(source, target):
        copies.append(pltpu.make_async_copy(source, target, sems.at[len(copies)]))
        copies[-1].start()

    put(block_ref, copy_hbm.at[:, pl.ds(pl.multiple_of(place(0, 0) * rows, rows), rows)])
    put(attn_ref, attn_hbm)
    put(cols_ref, cols_hbm)
    put(attn_cols_ref, attn_cols_hbm)
    row_factors = new_rows(got_ref, 0, rows // 2)
    rows_ref[...] = row_factors.reshape(rows)
    attn_rows_ref[...] = new_rows(got_ref, 1, rows // 2).reshape(rows)
    along = jnp.broadcast_to(lax.rsqrt(cols_ref[...].reshape(1, cols)), (SLAB, cols))
    scale = factor(got_ref, 0, count)
    row_scale = lax.rsqrt(row_factors)
    for b in range(blocks):
        across = down(row_scale[:, b * LANES : (b + 1) * LANES] * scale)
        for s in range(LANES // SLAB):
            at = pl.ds(b * LANES + s * SLAB, SLAB)
            new_ref[at, :] = (
                p_ref[at, :] - g_ref[at, :].astype(F32) * wide(across[s * SLAB : (s + 1) * SLAB], cols) * along
            )
        at = pl.ds(b * LANES, LANES)
        put(new_ref.at[at], new_hbm.at[at])
    put(rows_ref, rows_hbm)
    put(attn_rows_ref, attn_rows_hbm)
    for copy in copies:
        copy.wait()


def everyone(value, axes):
    return lax.all_to_all(value, axes, 0, 0, tiled=True)


def moved(value, dx, dy):
    xs, ys = lax.axis_size("row_0"), lax.axis_size("row_1")
    steps = {NEAR: (1, xs - 1), FAR: (xs - 1, 1)}.get(dx, (dx, dx))
    pairs = [(x * ys + y, (x + steps[x % 2]) % xs * ys + (y + dy) % ys) for x in range(xs) for y in range(ys)]
    return lax.ppermute(value, ROW, pairs)


def other_core(value):
    return lax.ppermute(value, CORE, [(0, 1), (1, 0)])


def step(
    mlp_param,
    mlp_grad,
    mlp_row_state,
    mlp_col_state,
    attn_param,
    attn_grad,
    attn_row_state,
    attn_col_state,
):
    rows, cols = mlp_grad.shape
    attn_cols = attn_grad.shape[1]
    half = rows // 2
    row_devices, layers = lax.axis_size(ROW), lax.axis_size(LAYERS)
    message = -(-(cols + attn_cols) // LANES) * LANES
    rows_total = rows * row_devices
    widths = (float(cols * lax.axis_size(COL)), float(attn_cols * lax.axis_size(COL)))
    counts = (rows_total * widths[0], rows_total * widths[1])
    attn_grad, attn_param = attn_grad.T, attn_param.T
    blocks = rows // LANES

    sent, row_sums, p_sums, g, ga, p, pa = call(
        sums_kernel,
        [
            pltpu.VMEM((row_devices, 1, message), F32),
            pltpu.VMEM((1, 2 * rows), F32),
            pltpu.VMEM((1, 2 * LANES), F32),
            pltpu.VMEM((rows, cols), BF16),
            pltpu.VMEM((attn_cols, rows), BF16),
            pltpu.VMEM((rows, cols), F32),
            pltpu.VMEM((attn_cols, rows), F32),
        ],
        (mlp_grad, attn_grad, mlp_param, attn_param),
        in_specs=[OFF_CHIP] * 4,
        scratch=[
            pltpu.VMEM((rows + 2 * LANES, LANES), F32),
            pltpu.SemaphoreType.DMA((2 * blocks + 2,)),
        ],
        limit=118 << 19,
    )
    got = everyone(sent, ROW)
    cols_new, attn_cols_new, kept, sent, ahead = call(
        functools.partial(columns_kernel, float(rows_total)),
        [
            pltpu.VMEM((cols,), F32),
            pltpu.VMEM((attn_cols,), F32),
            pltpu.VMEM((1, 4 * half), F32),
            pltpu.VMEM((1, 4 * half), F32),
            pltpu.VMEM((3 * attn_cols, rows), BF16),
        ],
        (got, row_sums, g, ga, pa, mlp_col_state, attn_col_state),
        scratch=[pltpu.VMEM((rows, LANES), F32)],
    )
    swapped = other_core(sent)
    (sent,) = call(
        spread_kernel,
        [pltpu.VMEM((layers, 1, 4 * half + 2 * LANES), F32)],
        (kept, swapped, p_sums),
    )
    got = everyone(sent, LAYERS)
    (sent,) = call(
        functools.partial(rows_kernel, widths),
        [pltpu.VMEM((2 * row_devices, 1, 4 * LANES + 2 * half), F32)],
        (got, mlp_row_state, attn_row_state),
    )
    got = everyone(sent, (*ROW, CORE))
    ahead = moved(ahead, 2, 0)
    attn_new, block, *parts = call(
        functools.partial(attn_kernel, counts[1]),
        [
            pltpu.VMEM((attn_cols, rows), F32),
            pltpu.VMEM((attn_cols, rows), BF16),
            *[pltpu.VMEM((attn_cols // 2, rows), BF16)] * 2,
        ],
        (got, attn_cols_new, ga, pa),
    )
    (across,) = call(
        functools.partial(early_kernel, counts[1]),
        [pltpu.VMEM((attn_cols, rows), BF16)],
        (got, attn_cols_new, ahead),
    )
    partner = moved(parts[0], 0, 1)
    partner_last = moved(parts[1], 0, 1)
    near = moved(block, NEAR, 0)
    far = moved(block, FAR, 0)
    partner_across = moved(across, 0, 1)
    partner_near = moved(partner, NEAR, 0)
    partner_far = moved(partner, FAR, 0)
    last_near = moved(partner_last, NEAR, 0)
    last_far = moved(partner_last, FAR, 0)
    copy, attn_new, mlp_new, rows_new, cols_new, attn_rows_new, attn_cols_new = call(
        functools.partial(finish_kernel, counts[0]),
        [
            jax.ShapeDtypeStruct((attn_cols, rows_total), BF16),
            jax.ShapeDtypeStruct((attn_cols, rows), F32),
            jax.ShapeDtypeStruct((rows, cols), F32),
            jax.ShapeDtypeStruct((rows,), F32),
            jax.ShapeDtypeStruct((cols,), F32),
            jax.ShapeDtypeStruct((rows,), F32),
            jax.ShapeDtypeStruct((attn_cols,), F32),
        ],
        (block, got, cols_new, attn_cols_new, attn_new, g, p),
        out_specs=[OFF_CHIP] * 7,
        scratch=[
            pltpu.VMEM((rows, cols), F32),
            pltpu.VMEM((rows,), F32),
            pltpu.VMEM((rows,), F32),
            pltpu.SemaphoreType.DMA((blocks + 6,)),
        ],
        flops=1 << 22,
    )
    copy = fill(
        copy,
        ((2, 0, 0), (0, 1, 0), (0, 1, attn_cols // 2), (NEAR, 0, 0), (FAR, 0, 0)),
        (across, partner, partner_last, near, far),
    )
    copy = fill(copy, ((2, 1, 0), (NEAR, 1, 0), (FAR, 1, 0)), (partner_across, partner_near, partner_far))
    copy = fill(copy, ((NEAR, 1, attn_cols // 2), (FAR, 1, attn_cols // 2)), (last_near, last_far))
    return mlp_new, attn_new.T, rows_new, cols_new, attn_rows_new, attn_cols_new, copy.T


def solution(mesh):
    finer = Mesh(mesh.devices.reshape(4, 2, 2, 8, 2), (*ROW, *COL))
    return jax.shard_map(
        step,
        mesh=finer,
        in_specs=(
            P(ROW, COL),
            P(ROW, COL),
            P(ROW),
            P(COL),
            P(ROW, COL),
            P(ROW, COL),
            P(ROW),
            P(COL),
        ),
        out_specs=(P(ROW, COL), P(ROW, COL), P(ROW), P(COL), P(ROW), P(COL), P(None, COL)),
        check_vma=False,
    )
```
